8 devices in a mesh: rep: 2 (over y, z), dp: 4 (over x, core).
Axes of the slice: x: 2, y: 2, z: 1, core: 2. Of those that a mesh axis runs over, the one named last changes fastest.
Arguments:
- x: bfloat16 [8, 2048, 1024], P(('rep', 'dp')), parts along dimension 0
- dy: bfloat16 [8, 2048, 1024], P(('rep', 'dp')), parts along dimension 0
- wq: bfloat16 [2, 1024, 1024], P(None, 'dp')
- wk: bfloat16 [2, 1024, 1024], P(None, 'dp')
- wv: bfloat16 [2, 1024, 1024], P(None, 'dp')
- wo: bfloat16 [2, 1024, 1024], P(None, 'dp')
- w_gate: bfloat16 [2, 1024, 4096], P(None, 'dp')
- w_up: bfloat16 [2, 1024, 4096], P(None, 'dp')
- w_down: bfloat16 [2, 4096, 1024], P(None, 'dp')
Outputs:
- output 1: bfloat16 [8, 2048, 1024], P(('rep', 'dp')), parts along dimension 0
- output 2: bfloat16 [4, 1024, 1024], P('rep', 'dp'), parts along dimension 0
- output 3: bfloat16 [4, 1024, 1024], P('rep', 'dp'), parts along dimension 0
- output 4: bfloat16 [4, 1024, 1024], P('rep', 'dp'), parts along dimension 0
- output 5: bfloat16 [4, 1024, 1024], P('rep', 'dp'), parts along dimension 0
- output 6: bfloat16 [4, 1024, 4096], P('rep', 'dp'), parts along dimension 0
- output 7: bfloat16 [4, 1024, 4096], P('rep', 'dp'), parts along dimension 0
- output 8: bfloat16 [4, 4096, 1024], P('rep', 'dp'), parts along dimension 0
There are 2 independent parts. The reference program is written for one: setup_inputs(seed, part) draws one part's arguments, and reference() takes and returns one part's arrays. A program takes and returns all parts, laid end to end along the dimension named above; an argument that names none is the same for every part.
All inputs are finite; a program needn't handle non-finite values.
Results may differ from the reference program's by a relative error of at most 0.029.
Values are sent between devices in bfloat16 or wider.
A program may use at most 2 GiB of HBM per device.

```python
import jax
import jax.numpy as jnp
from jax import lax

SEQUENCES = 4
TOKENS = 2048
D = 1024
HEADS = 8
KV_HEADS = 8
HEAD = 128
FF = 4096
LAYERS = 2
THETA = 10000
NAMES = ("wq", "wk", "wv", "wo", "w_gate", "w_up", "w_down")
SHAPES = {
    "wq": (LAYERS, D, HEADS * HEAD),
    "wk": (LAYERS, D, KV_HEADS * HEAD),
    "wv": (LAYERS, D, KV_HEADS * HEAD),
    "wo": (LAYERS, HEADS * HEAD, D),
    "w_gate": (LAYERS, D, FF),
    "w_up": (LAYERS, D, FF),
    "w_down": (LAYERS, FF, D),
}


def bump(key, n, height):
    away = (jnp.arange(n, dtype=jnp.int32) - jax.random.randint(key, (), 0, n, jnp.int32)) % n
    return jnp.where(away < n // 8, height, 1.0)


def together(key, own, strength):
    shared = jax.random.normal(key, own.shape[1:], jnp.float32)
    return (own + strength * shared) * lax.rsqrt(1 + strength * strength)


def setup_inputs(seed: int = 0, part: int = 0) -> dict:
    kx, kdy, ka, kb, kz, kf, kh, kl, *keys = jax.random.split(jax.random.key(seed), 8 + 3 * len(NAMES))
    kx, kdy, ka, kb = (jax.random.fold_in(k, part) for k in (kx, kdy, ka, kb))
    kw, km, kv = (keys[i::3] for i in range(3))
    shape = (SEQUENCES, TOKENS, D)
    much_x, much_dy = jax.random.uniform(kz, (2,), jnp.float32, 0.0, 1.0)
    loud = 2.0 ** jax.random.uniform(jax.random.fold_in(kz, 1), (), jnp.float32, -1.0, 2.0)
    layers = 2.0 ** jax.random.uniform(kl, (LAYERS, 1, 1), jnp.float32, -1.0, 1.0)
    times = {"wq": 1.0, "wk": 1.0, "wv": 2.0, "wo": layers, "w_gate": 1.0, "w_up": bump(kh, FF, 4.0), "w_down": layers}
    x = together(ka, jax.random.normal(kx, shape, jnp.float32), much_x) * bump(kf, D, 4.0)
    dy = together(kb, jax.random.normal(kdy, shape, jnp.float32), much_dy)
    drawn = {"x": x.astype(jnp.bfloat16), "dy": (loud * dy * (SEQUENCES * TOKENS) ** -0.5).astype(jnp.bfloat16)}
    for key, name in zip(kw, NAMES, strict=True):
        drawn[name] = (jax.random.normal(key, SHAPES[name], jnp.float32) * SHAPES[name][1] ** -0.5 * times[name]).astype(jnp.bfloat16)
    return drawn


def matmul(a, w):
    return jnp.dot(a, w, preferred_element_type=jnp.float32).astype(jnp.bfloat16)


def normed(h):
    wide = h.astype(jnp.float32)
    scale = lax.rsqrt(jnp.mean(wide**2, -1, keepdims=True) + 1e-6)
    return (wide * scale).astype(jnp.bfloat16)


def turned(t, theta):
    half = t.shape[-1] // 2
    angle = jnp.arange(t.shape[0], dtype=jnp.float32)[:, None] * theta ** (-jnp.arange(half, dtype=jnp.float32) / half)
    cos, sin = jnp.cos(angle)[:, None], jnp.sin(angle)[:, None]
    a, b = t[..., :half].astype(jnp.float32), t[..., half:].astype(jnp.float32)
    return jnp.concatenate([a * cos - b * sin, b * cos + a * sin], -1).astype(jnp.bfloat16)


def seen_by(q, k, v):
    tokens, kv = q.shape[0], k.shape[1]
    q = q.reshape(tokens, kv, -1, q.shape[-1])
    scores = jnp.einsum("tgsd,ugd->gstu", q.astype(jnp.float32), k.astype(jnp.float32)) * q.shape[-1] ** -0.5
    place = jnp.arange(tokens)
    weights = jax.nn.softmax(jnp.where(place[:, None] >= place, scores, -jnp.inf), -1).astype(jnp.bfloat16)
    return jnp.einsum("gstu,ugd->tgsd", weights.astype(jnp.float32), v.astype(jnp.float32)).astype(jnp.bfloat16).reshape(tokens, -1)


def layer(h, w):
    a = normed(h)
    q, k = (turned(matmul(a, w[name]).reshape(h.shape[0], -1, HEAD), THETA) for name in ("wq", "wk"))
    h = h + matmul(seen_by(q, k, matmul(a, w["wv"]).reshape(h.shape[0], -1, HEAD)), w["wo"])
    b = normed(h)
    gate = jnp.dot(b, w["w_gate"], preferred_element_type=jnp.float32)
    up = jnp.dot(b, w["w_up"], preferred_element_type=jnp.float32)
    return h + matmul((jax.nn.silu(gate) * up).astype(jnp.bfloat16), w["w_down"])


def stack(weights, h):
    return lax.scan(lambda h, w: (layer(h, w), None), h, weights)[0]


def reference(x, dy, wq, wk, wv, wo, w_gate, w_up, w_down):
    weights = dict(zip(NAMES, (wq, wk, wv, wo, w_gate, w_up, w_down), strict=True))

    def take(so_far, sequence):
        h, by_y = sequence
        _, back = jax.vjp(stack, weights, h)
        by_weights, by_h = back(by_y)
        return jax.tree.map(lambda total, term: total + term.astype(jnp.float32), so_far, by_weights), by_h

    none_yet = {name: jnp.zeros(w.shape, jnp.float32) for name, w in weights.items()}
    by_weights, by_x = lax.scan(take, none_yet, (x, dy))
    return (by_x, *(by_weights[name].astype(jnp.bfloat16) for name in NAMES))
```

```python
import jax
import jax.numpy as jnp
from jax import lax
from jax.experimental import pallas as pl
from jax.experimental.pallas import tpu as pltpu
from jax.sharding import PartitionSpec as P

HEAD = 128
THETA = 10000
EPS = 1e-6
NEG = -1e30
LOG2E = 1.4426950408889634
VMEM = 60 * 2**20
GROUP = 4
BLOCK = 512


def _dot(a, b, ca, cb):
    return lax.dot_general(a, b, (((ca,), (cb,)), ((), ())), preferred_element_type=jnp.float32)


def _turn(t, cos, sin):
    return t * cos + pltpu.roll(t, HEAD // 2, 1) * sin


def _turn_back(t, cos, sin):
    return t * cos + pltpu.roll(t * sin, HEAD // 2, 1)


def _hide(s, first_query, first_key):
    query = lax.broadcasted_iota(jnp.int32, s.shape, 1) + first_query
    key = lax.broadcasted_iota(jnp.int32, s.shape, 0) + first_key
    return query >= key


def _attend(q_ref, k_ref, v_ref, cos_ref, sin_ref, o_ref, lse_ref, qr, kr, top_s, mix_s, *, scale):
    iq = pl.program_id(1)
    e = scale * LOG2E
    rows = pl.ds(pl.multiple_of(iq * BLOCK, BLOCK), BLOCK)
    cos, sin = cos_ref[rows, :], sin_ref[rows, :]
    for i in range(GROUP):
        at = slice(i * HEAD, (i + 1) * HEAD)
        kr[rows, at] = _turn(k_ref[rows, at].astype(jnp.float32), cos, sin).astype(jnp.bfloat16)
        qr[:, at] = _turn(q_ref[:, at].astype(jnp.float32), cos, sin).astype(jnp.bfloat16)
    top_s[...] = jnp.full(top_s.shape, NEG, jnp.float32)
    mix_s[...] = jnp.zeros(mix_s.shape, jnp.float32)

    def block(first_key, keys, first_query, masked):
        here = pl.ds(first_key, keys)
        ones = jnp.ones((8, keys), jnp.bfloat16)
        cols = slice(first_query, BLOCK)
        scores = [_dot(kr[here, i * HEAD : (i + 1) * HEAD], qr[cols, i * HEAD : (i + 1) * HEAD], 1, 1) for i in range(GROUP)]
        ok = _hide(scores[0], 0, 0) if masked else None
        weights, keeps = [], []
        for i, s in enumerate(scores):
            if masked:
                s = jnp.where(ok, s, 2 * NEG)
            old = top_s[i : i + 1, cols]
            top = jnp.maximum(old, s.max(axis=0, keepdims=True))
            top_s[i : i + 1, cols] = top
            weights.append(jnp.exp2((s - top) * e).astype(jnp.bfloat16))
            keeps.append(jnp.exp2((old - top) * e))
        for i, (p, keep) in enumerate(zip(weights, keeps)):
            values = jnp.concatenate([v_ref[here, i * HEAD : (i + 1) * HEAD].T, ones], axis=0)
            mix_s[i, :, cols] = mix_s[i, :, cols] * keep + _dot(values, p, 1, 0)

    lax.fori_loop(0, iq, lambda j, _: block(pl.multiple_of(j * BLOCK, BLOCK), BLOCK, 0, False), None)
    for n in range(0, BLOCK, 256):
        block(pl.multiple_of(iq * BLOCK + n, 256), 256, n, True)
    for i in range(GROUP):
        total = mix_s[i, HEAD : HEAD + 1, :]
        o_ref[:, i * HEAD : (i + 1) * HEAD] = (mix_s[i, :HEAD, :] * (1 / total)).T.astype(jnp.bfloat16)
        lse_ref[0, i : i + 1, :] = top_s[i : i + 1, :] * scale + jnp.log(total)


def attend(qkv, cos, sin):
    tokens, wide = qkv.shape[0], GROUP * HEAD
    groups = qkv.shape[1] // (3 * wide)
    table = pl.BlockSpec((tokens, HEAD), lambda g, i: (0, 0))
    return pl.pallas_call(
        lambda *refs: _attend(*refs, scale=HEAD**-0.5),
        grid=(groups, tokens // BLOCK),
        in_specs=[
            pl.BlockSpec((BLOCK, wide), lambda g, i: (i, 3 * g)),
            pl.BlockSpec((tokens, wide), lambda g, i: (0, 3 * g + 1)),
            pl.BlockSpec((tokens, wide), lambda g, i: (0, 3 * g + 2)),
            table,
            table,
        ],
        out_specs=[pl.BlockSpec((BLOCK, wide), lambda g, i: (i, g)), pl.BlockSpec((1, GROUP, BLOCK), lambda g, i: (g, 0, i))],
        out_shape=[
            jax.ShapeDtypeStruct((tokens, groups * wide), jnp.bfloat16),
            jax.ShapeDtypeStruct((groups, GROUP, tokens), jnp.float32),
        ],
        scratch_shapes=[
            pltpu.VMEM((BLOCK, wide), jnp.bfloat16),
            pltpu.VMEM((tokens, wide), jnp.bfloat16),
            pltpu.VMEM((8, BLOCK), jnp.float32),
            pltpu.VMEM((GROUP, HEAD + 8, BLOCK), jnp.float32),
        ],
        compiler_params=pltpu.CompilerParams(dimension_semantics=("arbitrary", "arbitrary"), vmem_limit_bytes=VMEM),
        cost_estimate=pl.CostEstimate(flops=30 * 10**9, transcendentals=20 * 10**6, bytes_accessed=20 * 2**20),
        name="attend",
    )(qkv, qkv, qkv, cos, sin)


def _attend_bwd(q_ref, k_ref, v_ref, o_ref, do_ref, lse_ref, cos_ref, sin_ref, d_ref, qr, kr, dq_s, dk_s, dv_s, *, scale):
    iq, last = pl.program_id(1), pl.num_programs(1) - 1
    e = scale * LOG2E
    wide = GROUP * HEAD
    rows = pl.ds(pl.multiple_of(iq * BLOCK, BLOCK), BLOCK)
    cos, sin = cos_ref[rows, :], sin_ref[rows, :]
    lses, deltas = [], []
    for i in range(GROUP):
        at = slice(i * HEAD, (i + 1) * HEAD)
        kr[rows, at] = _turn(k_ref[rows, at].astype(jnp.float32), cos, sin).astype(jnp.bfloat16)
        qr[:, at] = _turn(q_ref[:, at].astype(jnp.float32), cos, sin).astype(jnp.bfloat16)
        lses.append(lse_ref[0, i : i + 1, :] * LOG2E)
        deltas.append((do_ref[:, at].astype(jnp.float32) * o_ref[:, at].astype(jnp.float32)).T.sum(axis=0, keepdims=True))
    dq_s[...] = jnp.zeros(dq_s.shape, jnp.float32)
    dk_s[rows, :] = jnp.zeros((BLOCK, wide), jnp.float32)
    dv_s[rows, :] = jnp.zeros((BLOCK, wide), jnp.float32)

    def block(first_key, keys, first_query, masked):
        here = pl.ds(first_key, keys)
        cols = slice(first_query, BLOCK)
        heads = [slice(i * HEAD, (i + 1) * HEAD) for i in range(GROUP)]
        scores = [_dot(kr[here, at], qr[cols, at], 1, 1) for at in heads]
        dps = [_dot(v_ref[here, at], do_ref[cols, at], 1, 1) for at in heads]
        ok = _hide(scores[0], 0, 0) if masked else None
        for i, at in enumerate(heads):
            p = jnp.exp2(scores[i] * e - lses[i][:, cols])
            if masked:
                p = jnp.where(ok, p, 0.0)
            ds = (p * (dps[i] - deltas[i][:, cols])).astype(jnp.bfloat16)
            dv_s[here, at] += _dot(p.astype(jnp.bfloat16), do_ref[cols, at], 1, 0)
            dk_s[here, at] += _dot(ds, qr[cols, at], 1, 0)
            dq_s[i, :, cols] += _dot(kr[here, at].T, ds, 1, 0)

    lax.fori_loop(0, iq, lambda j, _: block(pl.multiple_of(j * BLOCK, BLOCK), BLOCK, 0, False), None)
    for n in range(0, BLOCK, 256):
        block(pl.multiple_of(iq * BLOCK + n, 256), 256, n, True)

    def narrow(t):
        return t.astype(jnp.bfloat16).astype(jnp.float32)

    for i in range(GROUP):
        at = slice(i * HEAD, (i + 1) * HEAD)
        d_ref[rows, at] = _turn_back(narrow((dq_s[i] * scale).T), cos, sin).astype(jnp.bfloat16)

    @pl.when(iq == last)
    def _():
        def finish(n, _):
            here = pl.ds(pl.multiple_of(n * BLOCK, BLOCK), BLOCK)
            c, s = cos_ref[here, :], sin_ref[here, :]
            for i in range(GROUP):
                at = slice(i * HEAD, (i + 1) * HEAD)
                d_ref[here, wide + i * HEAD : wide + (i + 1) * HEAD] = _turn_back(narrow(dk_s[here, at] * scale), c, s).astype(jnp.bfloat16)
            d_ref[here, 2 * wide :] = dv_s[here, :].astype(jnp.bfloat16)

        lax.fori_loop(0, last + 1, finish, None)


def attend_bwd(qkv, o, do, lse, cos, sin):
    tokens, wide = qkv.shape[0], GROUP * HEAD
    groups = qkv.shape[1] // (3 * wide)
    table = pl.BlockSpec((tokens, HEAD), lambda g, i: (0, 0))
    own = pl.BlockSpec((BLOCK, wide), lambda g, i: (i, g))
    return pl.pallas_call(
        lambda *refs: _attend_bwd(*refs, scale=HEAD**-0.5),
        grid=(groups, tokens // BLOCK),
        in_specs=[
            pl.BlockSpec((BLOCK, wide), lambda g, i: (i, 3 * g)),
            pl.BlockSpec((tokens, wide), lambda g, i: (0, 3 * g + 1)),
            pl.BlockSpec((tokens, wide), lambda g, i: (0, 3 * g + 2)),
            own,
            own,
            pl.BlockSpec((1, GROUP, BLOCK), lambda g, i: (g, 0, i)),
            table,
            table,
        ],
        out_specs=pl.BlockSpec((tokens, 3 * wide), lambda g, i: (0, g)),
        out_shape=jax.ShapeDtypeStruct(qkv.shape, jnp.bfloat16),
        scratch_shapes=[
            pltpu.VMEM((BLOCK, wide), jnp.bfloat16),
            pltpu.VMEM((tokens, wide), jnp.bfloat16),
            pltpu.VMEM((GROUP, HEAD, BLOCK), jnp.float32),
            pltpu.VMEM((tokens, wide), jnp.float32),
            pltpu.VMEM((tokens, wide), jnp.float32),
        ],
        compiler_params=pltpu.CompilerParams(dimension_semantics=("arbitrary", "arbitrary"), vmem_limit_bytes=VMEM),
        cost_estimate=pl.CostEstimate(flops=60 * 10**9, transcendentals=20 * 10**6, bytes_accessed=40 * 2**20),
        name="attend_bwd",
    )(qkv, qkv, qkv, o, do, lse, cos, sin)


def _up(b_ref, wg_ref, wu_ref, gate_ref, up_ref, act_ref, *, rows):
    def some(n, _):
        here = pl.ds(pl.multiple_of(n * rows, rows), rows)
        b = b_ref[here, :]
        gate, up = _dot(b, wg_ref[...], 1, 0), _dot(b, wu_ref[...], 1, 0)
        gate_ref[here, :] = gate
        up_ref[here, :] = up
        act_ref[here, :] = (gate * jax.nn.sigmoid(gate) * up).astype(jnp.bfloat16)

    lax.fori_loop(0, b_ref.shape[0] // rows, some, None, unroll=True)


def ffn_up(b, w_gate, w_up, tile=256, rows=512):
    (tokens, d), ff = b.shape, w_gate.shape[1]
    weight = pl.BlockSpec((d, tile), lambda j: (0, j))
    out = pl.BlockSpec((tokens, tile), lambda j: (0, j))
    return pl.pallas_call(
        lambda *refs: _up(*refs, rows=rows),
        grid=(ff // tile,),
        in_specs=[pl.BlockSpec((tokens, d), lambda j: (0, 0)), weight, weight],
        out_specs=[out, out, out],
        out_shape=[jax.ShapeDtypeStruct((tokens, ff), t) for t in (jnp.float32, jnp.float32, jnp.bfloat16)],
        compiler_params=pltpu.CompilerParams(dimension_semantics=("arbitrary",), vmem_limit_bytes=VMEM),
        cost_estimate=pl.CostEstimate(flops=4 * tokens * d * ff, transcendentals=tokens * ff, bytes_accessed=10 * tokens * ff + 4 * d * ff),
        name="ffn_up",
    )(b, w_gate, w_up)


def _down_bwd(dh_ref, wd_ref, gate_ref, up_ref, dg_ref, du_ref, *, rows):
    def some(n, _):
        here = pl.ds(pl.multiple_of(n * rows, rows), rows)
        dact = _dot(dh_ref[here, :], wd_ref[...], 1, 1).astype(jnp.bfloat16).astype(jnp.float32)
        gate, up = gate_ref[here, :], up_ref[here, :]
        s = jax.nn.sigmoid(gate)
        silu = gate * s
        du_ref[here, :] = (dact * silu).astype(jnp.bfloat16)
        dg_ref[here, :] = (dact * up * (s + silu * (1 - s))).astype(jnp.bfloat16)

    lax.fori_loop(0, dh_ref.shape[0] // rows, some, None, unroll=True)


def ffn_down_bwd(dh, w_down, gate, up, tile=256, rows=512):
    (tokens, d), ff = dh.shape, w_down.shape[0]
    cut = pl.BlockSpec((tokens, tile), lambda j: (0, j))
    return pl.pallas_call(
        lambda *refs: _down_bwd(*refs, rows=rows),
        grid=(ff // tile,),
        in_specs=[pl.BlockSpec((tokens, d), lambda j: (0, 0)), pl.BlockSpec((tile, d), lambda j: (j, 0)), cut, cut],
        out_specs=[cut, cut],
        out_shape=[jax.ShapeDtypeStruct((tokens, ff), jnp.bfloat16)] * 2,
        compiler_params=pltpu.CompilerParams(dimension_semantics=("arbitrary",), vmem_limit_bytes=VMEM),
        cost_estimate=pl.CostEstimate(flops=4 * tokens * d * ff, transcendentals=tokens * ff, bytes_accessed=12 * tokens * ff + 2 * d * ff),
        name="ffn_down_bwd",
    )(dh, w_down, gate, up)


def matmul(a, w):
    return jnp.dot(a, w, preferred_element_type=jnp.float32).astype(jnp.bfloat16)


def matmul_nt(a, w):
    return _dot(a, w, 1, 1).astype(jnp.bfloat16)


def matmul_tn(a, b):
    return _dot(a, b, 0, 0).astype(jnp.bfloat16)


def norm_scale(h):
    return lax.rsqrt(jnp.mean(h.astype(jnp.float32) ** 2, -1, keepdims=True) + EPS)


def normed(h):
    return (h.astype(jnp.float32) * norm_scale(h)).astype(jnp.bfloat16)


def normed_bwd(h, da, dh):
    wide, da = h.astype(jnp.float32), da.astype(jnp.float32)
    scale = norm_scale(h)
    inner = jnp.sum(da * wide, -1, keepdims=True) * (scale**3 / h.shape[-1])
    return (dh.astype(jnp.float32) + (da * scale - wide * inner).astype(jnp.bfloat16).astype(jnp.float32)).astype(jnp.bfloat16)


def tables(tokens):
    half = HEAD // 2
    angle = jnp.arange(tokens, dtype=jnp.float32)[:, None] * THETA ** (-jnp.arange(half, dtype=jnp.float32) / half)
    cos, sin = jnp.cos(angle), jnp.sin(angle)
    return jnp.concatenate([cos, cos], -1), jnp.concatenate([-sin, sin], -1)


def interleaved(q, k, v):
    wide = GROUP * HEAD
    return [t[:, a : a + wide] for a in range(0, q.shape[1], wide) for t in (q, k, v)]


def parted(t):
    wide = GROUP * HEAD
    return [jnp.concatenate([t[:, a : a + wide] for a in range(n * wide, t.shape[1], 3 * wide)], axis=1) for n in range(3)]


def together(first, *rest):
    return lax.optimization_barrier((first, *rest))


def solution(mesh):
    reps = mesh.shape["rep"]

    def step(x, dy, *weights):
        layers = weights[0].shape[0]
        rep = lax.axis_index("rep")
        cos, sin = tables(x.shape[1])

        def mine(w, number):
            part = w.shape[1] // reps
            return lax.dynamic_slice(w, (number, rep * part, 0), (1, part, w.shape[2]))[0]

        def whole(shard):
            return lax.all_gather(shard, ("dp", "rep"), axis=0, tiled=True)

        def scatter(term):
            return lax.psum_scatter(term, "dp", scatter_dimension=0, tiled=True)

        fetched = []
        for n in range(layers):
            wq, wk, wv, wo, wg, wu, wd = (mine(w, n) for w in weights)
            square = whole(jnp.concatenate([*interleaved(wq, wk, wv), wo], axis=1))
            fetched.append((square, whole(wg), whole(wu), whole(wd)))
        three = 3 * weights[0].shape[2]

        h, kept = x[0], []
        for n in range(layers):
            square, wg, wu, wd = fetched[n]
            a = normed(h)
            qkv = matmul(a, square[:, :three])
            o, lse = attend(qkv, cos, sin)
            h1 = h + matmul(o, square[:, three:])
            b = normed(h1)
            gate, up, act = ffn_up(b, wg, wu)
            kept.append((h, a, qkv, o, lse, h1, b, gate, up, act))
            if n < layers - 1:
                h = h1 + matmul(act, wd)

        dh, grads, sums, out = dy[0], [None] * layers, {}, {}

        def after(value, *keys):
            for key in keys:
                if key in sums:
                    value, out[key] = together(value, sums.pop(key))
            return value

        for n in reversed(range(layers)):
            square, wg, wu, wd = fetched[n]
            h, a, qkv, o, lse, h1, b, gate, up, act = kept[n]
            d_down = matmul_tn(act, dh)
            dh, d_down = together(dh, d_down)
            sums["down", n] = scatter(d_down)
            dg, du = ffn_down_bwd(dh, wd, gate, up)
            dg = after(dg, ("qkv", n + 1))
            d_gate = matmul_tn(b, dg)
            sums["gate", n] = scatter(d_gate)
            dg, du, d_gate = together(dg, du, d_gate)
            du = after(du, ("down", n))
            d_up = matmul_tn(b, du)
            dg, du, d_up = together(dg, du, d_up)
            sums["up", n] = scatter(d_up)
            db = matmul_nt(dg, wg) + matmul_nt(du, wu)
            dh1 = after(normed_bwd(h1, db, dh), ("gate", n))
            d_o = matmul_tn(o, dh1)
            dh1, d_o = together(dh1, d_o)
            sums["o", n] = scatter(d_o)
            do = matmul_nt(dh1, square[:, three:])
            dqkv = after(attend_bwd(qkv, o, do, lse, cos, sin), ("up", n))
            d_qkv = matmul_tn(a, dqkv)
            dqkv, d_qkv = together(dqkv, d_qkv)
            dqkv = after(dqkv, ("o", n))
            sums["qkv", n] = scatter(d_qkv)
            dh = normed_bwd(h, matmul_nt(dqkv, square[:, :three]), dh1)
        out |= sums
        grads = [(*parted(out["qkv", n]), *(out[name, n] for name in ("o", "gate", "up", "down"))) for n in range(layers)]
        return (dh[None], *(jnp.stack([g[i] for g in grads]) for i in range(7)))

    states, cut = P(("rep", "dp"), None, None), P(None, "dp", None)
    return jax.shard_map(
        step,
        mesh=mesh,
        in_specs=(states, states) + (cut,) * 7,
        out_specs=(states,) + (P("rep", "dp", None),) * 7,
        check_vma=False,
    )
```

```python
import jax
import jax.numpy as jnp
from jax import lax
from jax.experimental import pallas as pl
from jax.experimental.pallas import tpu as pltpu
from jax.sharding import PartitionSpec as P

HEAD = 128
THETA = 10000
EPS = 1e-6
NEG = -1e30
LOG2E = 1.4426950408889634
VMEM = 60 * 2**20
GROUP = 4
BLOCK = 512


def _dot(a, b, ca, cb):
    return lax.dot_general(a, b, (((ca,), (cb,)), ((), ())), preferred_element_type=jnp.float32)


def _turn(t, cos, sin):
    return t * cos + pltpu.roll(t, HEAD // 2, 1) * sin


def _turn_back(t, cos, sin):
    return t * cos + pltpu.roll(t * sin, HEAD // 2, 1)


def _hide(s, first_query, first_key):
    query = lax.broadcasted_iota(jnp.int32, s.shape, 1) + first_query
    key = lax.broadcasted_iota(jnp.int32, s.shape, 0) + first_key
    return query >= key


def _attend(q_ref, k_ref, v_ref, cos_ref, sin_ref, o_ref, lse_ref, qr, kr, top_s, mix_s, *, scale):
    iq = pl.program_id(1)
    e = scale * LOG2E
    rows = pl.ds(pl.multiple_of(iq * BLOCK, BLOCK), BLOCK)
    cos, sin = cos_ref[rows, :], sin_ref[rows, :]
    for i in range(GROUP):
        at = slice(i * HEAD, (i + 1) * HEAD)
        kr[rows, at] = _turn(k_ref[rows, at].astype(jnp.float32), cos, sin).astype(jnp.bfloat16)
        qr[:, at] = _turn(q_ref[:, at].astype(jnp.float32), cos, sin).astype(jnp.bfloat16)
    top_s[...] = jnp.full(top_s.shape, NEG, jnp.float32)
    mix_s[...] = jnp.zeros(mix_s.shape, jnp.float32)

    def block(first_key, keys, first_query, masked):
        here = pl.ds(first_key, keys)
        ones = jnp.ones((8, keys), jnp.bfloat16)
        cols = slice(first_query, BLOCK)
        scores = [_dot(kr[here, i * HEAD : (i + 1) * HEAD], qr[cols, i * HEAD : (i + 1) * HEAD], 1, 1) for i in range(GROUP)]
        ok = _hide(scores[0], 0, 0) if masked else None
        weights, keeps = [], []
        for i, s in enumerate(scores):
            if masked:
                s = jnp.where(ok, s, 2 * NEG)
            old = top_s[i : i + 1, cols]
            top = jnp.maximum(old, s.max(axis=0, keepdims=True))
            top_s[i : i + 1, cols] = top
            weights.append(jnp.exp2((s - top) * e).astype(jnp.bfloat16))
            keeps.append(jnp.exp2((old - top) * e))
        for i, (p, keep) in enumerate(zip(weights, keeps)):
            values = jnp.concatenate([v_ref[here, i * HEAD : (i + 1) * HEAD].T, ones], axis=0)
            mix_s[i, :, cols] = mix_s[i, :, cols] * keep + _dot(values, p, 1, 0)

    lax.fori_loop(0, iq, lambda j, _: block(pl.multiple_of(j * BLOCK, BLOCK), BLOCK, 0, False), None)
    for n in range(0, BLOCK, 256):
        block(pl.multiple_of(iq * BLOCK + n, 256), 256, n, True)
    for i in range(GROUP):
        total = mix_s[i, HEAD : HEAD + 1, :]
        o_ref[:, i * HEAD : (i + 1) * HEAD] = (mix_s[i, :HEAD, :] * (1 / total)).T.astype(jnp.bfloat16)
        lse_ref[0, i : i + 1, :] = top_s[i : i + 1, :] * scale + jnp.log(total)


def attend(qkv, cos, sin):
    tokens, wide = qkv.shape[0], GROUP * HEAD
    groups = qkv.shape[1] // (3 * wide)
    table = pl.BlockSpec((tokens, HEAD), lambda g, i: (0, 0))
    return pl.pallas_call(
        lambda *refs: _attend(*refs, scale=HEAD**-0.5),
        grid=(groups, tokens // BLOCK),
        in_specs=[
            pl.BlockSpec((BLOCK, wide), lambda g, i: (i, 3 * g)),
            pl.BlockSpec((tokens, wide), lambda g, i: (0, 3 * g + 1)),
            pl.BlockSpec((tokens, wide), lambda g, i: (0, 3 * g + 2)),
            table,
            table,
        ],
        out_specs=[pl.BlockSpec((BLOCK, wide), lambda g, i: (i, g)), pl.BlockSpec((1, GROUP, BLOCK), lambda g, i: (g, 0, i))],
        out_shape=[
            jax.ShapeDtypeStruct((tokens, groups * wide), jnp.bfloat16),
            jax.ShapeDtypeStruct((groups, GROUP, tokens), jnp.float32),
        ],
        scratch_shapes=[
            pltpu.VMEM((BLOCK, wide), jnp.bfloat16),
            pltpu.VMEM((tokens, wide), jnp.bfloat16),
            pltpu.VMEM((8, BLOCK), jnp.float32),
            pltpu.VMEM((GROUP, HEAD + 8, BLOCK), jnp.float32),
        ],
        compiler_params=pltpu.CompilerParams(dimension_semantics=("arbitrary", "arbitrary"), vmem_limit_bytes=VMEM),
        cost_estimate=pl.CostEstimate(flops=30 * 10**9, transcendentals=20 * 10**6, bytes_accessed=20 * 2**20),
        name="attend",
    )(qkv, qkv, qkv, cos, sin)


def _attend_bwd(q_ref, k_ref, v_ref, o_ref, do_ref, lse_ref, cos_ref, sin_ref, d_ref, qr, kr, dq_s, dk_s, dv_s, *, scale):
    iq, last = pl.program_id(1), pl.num_programs(1) - 1
    e = scale * LOG2E
    wide = GROUP * HEAD
    rows = pl.ds(pl.multiple_of(iq * BLOCK, BLOCK), BLOCK)
    cos, sin = cos_ref[rows, :], sin_ref[rows, :]
    lses, deltas = [], []
    for i in range(GROUP):
        at = slice(i * HEAD, (i + 1) * HEAD)
        kr[rows, at] = _turn(k_ref[rows, at].astype(jnp.float32), cos, sin).astype(jnp.bfloat16)
        qr[:, at] = _turn(q_ref[:, at].astype(jnp.float32), cos, sin).astype(jnp.bfloat16)
        lses.append(lse_ref[0, i : i + 1, :] * LOG2E)
        deltas.append((do_ref[:, at].astype(jnp.float32) * o_ref[:, at].astype(jnp.float32)).T.sum(axis=0, keepdims=True))
    dq_s[...] = jnp.zeros(dq_s.shape, jnp.float32)
    dk_s[rows, :] = jnp.zeros((BLOCK, wide), jnp.float32)
    dv_s[rows, :] = jnp.zeros((BLOCK, wide), jnp.float32)

    def block(first_key, keys, first_query, masked):
        here = pl.ds(first_key, keys)
        cols = slice(first_query, BLOCK)
        heads = [slice(i * HEAD, (i + 1) * HEAD) for i in range(GROUP)]
        scores = [_dot(kr[here, at], qr[cols, at], 1, 1) for at in heads]
        dps = [_dot(v_ref[here, at], do_ref[cols, at], 1, 1) for at in heads]
        ok = _hide(scores[0], 0, 0) if masked else None
        for i, at in enumerate(heads):
            p = jnp.exp2(scores[i] * e - lses[i][:, cols])
            if masked:
                p = jnp.where(ok, p, 0.0)
            ds = (p * (dps[i] - deltas[i][:, cols])).astype(jnp.bfloat16)
            dv_s[here, at] += _dot(p.astype(jnp.bfloat16), do_ref[cols, at], 1, 0)
            dk_s[here, at] += _dot(ds, qr[cols, at], 1, 0)
            dq_s[i, :, cols] += _dot(kr[here, at].T, ds, 1, 0)

    lax.fori_loop(0, iq, lambda j, _: block(pl.multiple_of(j * BLOCK, BLOCK), BLOCK, 0, False), None)
    for n in range(0, BLOCK, 256):
        block(pl.multiple_of(iq * BLOCK + n, 256), 256, n, True)

    def narrow(t):
        return t.astype(jnp.bfloat16).astype(jnp.float32)

    for i in range(GROUP):
        at = slice(i * HEAD, (i + 1) * HEAD)
        d_ref[rows, at] = _turn_back(narrow((dq_s[i] * scale).T), cos, sin).astype(jnp.bfloat16)

    @pl.when(iq == last)
    def _():
        def finish(n, _):
            here = pl.ds(pl.multiple_of(n * BLOCK, BLOCK), BLOCK)
            c, s = cos_ref[here, :], sin_ref[here, :]
            for i in range(GROUP):
                at = slice(i * HEAD, (i + 1) * HEAD)
                d_ref[here, wide + i * HEAD : wide + (i + 1) * HEAD] = _turn_back(narrow(dk_s[here, at] * scale), c, s).astype(jnp.bfloat16)
            d_ref[here, 2 * wide :] = dv_s[here, :].astype(jnp.bfloat16)

        lax.fori_loop(0, last + 1, finish, None)


def attend_bwd(qkv, o, do, lse, cos, sin):
    tokens, wide = qkv.shape[0], GROUP * HEAD
    groups = qkv.shape[1] // (3 * wide)
    table = pl.BlockSpec((tokens, HEAD), lambda g, i: (0, 0))
    own = pl.BlockSpec((BLOCK, wide), lambda g, i: (i, g))
    return pl.pallas_call(
        lambda *refs: _attend_bwd(*refs, scale=HEAD**-0.5),
        grid=(groups, tokens // BLOCK),
        in_specs=[
            pl.BlockSpec((BLOCK, wide), lambda g, i: (i, 3 * g)),
            pl.BlockSpec((tokens, wide), lambda g, i: (0, 3 * g + 1)),
            pl.BlockSpec((tokens, wide), lambda g, i: (0, 3 * g + 2)),
            own,
            own,
            pl.BlockSpec((1, GROUP, BLOCK), lambda g, i: (g, 0, i)),
            table,
            table,
        ],
        out_specs=pl.BlockSpec((tokens, 3 * wide), lambda g, i: (0, g)),
        out_shape=jax.ShapeDtypeStruct(qkv.shape, jnp.bfloat16),
        scratch_shapes=[
            pltpu.VMEM((BLOCK, wide), jnp.bfloat16),
            pltpu.VMEM((tokens, wide), jnp.bfloat16),
            pltpu.VMEM((GROUP, HEAD, BLOCK), jnp.float32),
            pltpu.VMEM((tokens, wide), jnp.float32),
            pltpu.VMEM((tokens, wide), jnp.float32),
        ],
        compiler_params=pltpu.CompilerParams(dimension_semantics=("arbitrary", "arbitrary"), vmem_limit_bytes=VMEM),
        cost_estimate=pl.CostEstimate(flops=60 * 10**9, transcendentals=20 * 10**6, bytes_accessed=40 * 2**20),
        name="attend_bwd",
    )(qkv, qkv, qkv, o, do, lse, cos, sin)


def _up(b_ref, wg_ref, wu_ref, gate_ref, up_ref, act_ref, *, rows):
    def some(n, _):
        here = pl.ds(pl.multiple_of(n * rows, rows), rows)
        b = b_ref[here, :]
        gate, up = _dot(b, wg_ref[...], 1, 0), _dot(b, wu_ref[...], 1, 0)
        gate_ref[here, :] = gate
        up_ref[here, :] = up
        act_ref[here, :] = (gate * jax.nn.sigmoid(gate) * up).astype(jnp.bfloat16)

    lax.fori_loop(0, b_ref.shape[0] // rows, some, None, unroll=True)


def ffn_up(b, w_gate, w_up, tile=256, rows=512):
    (tokens, d), ff = b.shape, w_gate.shape[1]
    weight = pl.BlockSpec((d, tile), lambda j: (0, j))
    out = pl.BlockSpec((tokens, tile), lambda j: (0, j))
    return pl.pallas_call(
        lambda *refs: _up(*refs, rows=rows),
        grid=(ff // tile,),
        in_specs=[pl.BlockSpec((tokens, d), lambda j: (0, 0)), weight, weight],
        out_specs=[out, out, out],
        out_shape=[jax.ShapeDtypeStruct((tokens, ff), t) for t in (jnp.float32, jnp.float32, jnp.bfloat16)],
        compiler_params=pltpu.CompilerParams(dimension_semantics=("arbitrary",), vmem_limit_bytes=VMEM),
        cost_estimate=pl.CostEstimate(flops=4 * tokens * d * ff, transcendentals=tokens * ff, bytes_accessed=10 * tokens * ff + 4 * d * ff),
        name="ffn_up",
    )(b, w_gate, w_up)


def _down_bwd(dh_ref, wd_ref, gate_ref, up_ref, dg_ref, du_ref, *, rows):
    def some(n, _):
        here = pl.ds(pl.multiple_of(n * rows, rows), rows)
        dact = _dot(dh_ref[here, :], wd_ref[...], 1, 1).astype(jnp.bfloat16).astype(jnp.float32)
        gate, up = gate_ref[here, :], up_ref[here, :]
        s = jax.nn.sigmoid(gate)
        silu = gate * s
        du_ref[here, :] = (dact * silu).astype(jnp.bfloat16)
        dg_ref[here, :] = (dact * up * (s + silu * (1 - s))).astype(jnp.bfloat16)

    lax.fori_loop(0, dh_ref.shape[0] // rows, some, None, unroll=True)


def ffn_down_bwd(dh, w_down, gate, up, tile=256, rows=512):
    (tokens, d), ff = dh.shape, w_down.shape[0]
    cut = pl.BlockSpec((tokens, tile), lambda j: (0, j))
    return pl.pallas_call(
        lambda *refs: _down_bwd(*refs, rows=rows),
        grid=(ff // tile,),
        in_specs=[pl.BlockSpec((tokens, d), lambda j: (0, 0)), pl.BlockSpec((tile, d), lambda j: (j, 0)), cut, cut],
        out_specs=[cut, cut],
        out_shape=[jax.ShapeDtypeStruct((tokens, ff), jnp.bfloat16)] * 2,
        compiler_params=pltpu.CompilerParams(dimension_semantics=("arbitrary",), vmem_limit_bytes=VMEM),
        cost_estimate=pl.CostEstimate(flops=4 * tokens * d * ff, transcendentals=tokens * ff, bytes_accessed=12 * tokens * ff + 2 * d * ff),
        name="ffn_down_bwd",
    )(dh, w_down, gate, up)


def matmul(a, w):
    return jnp.dot(a, w, preferred_element_type=jnp.float32).astype(jnp.bfloat16)


def matmul_nt(a, w):
    return _dot(a, w, 1, 1).astype(jnp.bfloat16)


def matmul_tn(a, b):
    return _dot(a, b, 0, 0).astype(jnp.bfloat16)


def norm_scale(h):
    return lax.rsqrt(jnp.mean(h.astype(jnp.float32) ** 2, -1, keepdims=True) + EPS)


def normed(h):
    return (h.astype(jnp.float32) * norm_scale(h)).astype(jnp.bfloat16)


def normed_bwd(h, da, dh):
    wide, da = h.astype(jnp.float32), da.astype(jnp.float32)
    scale = norm_scale(h)
    inner = jnp.sum(da * wide, -1, keepdims=True) * (scale**3 / h.shape[-1])
    return (dh.astype(jnp.float32) + (da * scale - wide * inner).astype(jnp.bfloat16).astype(jnp.float32)).astype(jnp.bfloat16)


def tables(tokens):
    half = HEAD // 2
    angle = jnp.arange(tokens, dtype=jnp.float32)[:, None] * THETA ** (-jnp.arange(half, dtype=jnp.float32) / half)
    cos, sin = jnp.cos(angle), jnp.sin(angle)
    return jnp.concatenate([cos, cos], -1), jnp.concatenate([-sin, sin], -1)


CHUNKS = 4


def _exchange(refs, out, stage, sems, *, layer):
    loaded, own, sends, recvs = sems
    rep, dp = lax.axis_index("rep"), lax.axis_index("dp")
    x, core = dp // 2, dp % 2
    across = (rep, dp + 2 - 4 * x)
    group = (1 - rep, dp)
    partner = (rep, dp + 1 - 2 * core)
    rows = refs[0].shape[1]
    half = rows // 2
    part = half // CHUNKS
    wide = GROUP * HEAD
    square = refs[0].shape[2]

    def local():
        copies = []
        for a in range(0, square, wide):
            for i in range(3):
                copies.append((refs[i].at[layer, :, pl.ds(a, wide)], stage.at[:, pl.ds(3 * a + i * wide, wide)]))
        copies.append((refs[3].at[layer], stage.at[:, pl.ds(3 * square, refs[3].shape[2])]))
        return [pltpu.make_async_copy(s, d, loaded.at[n]) for n, (s, d) in enumerate(copies)]

    def remote(source, at, size, n, device):
        return pltpu.make_async_remote_copy(
            src_ref=source, dst_ref=out.at[pl.ds(at, size), :], send_sem=sends.at[n], recv_sem=recvs.at[n],
            device_id=device, device_id_type=pl.DeviceIdType.MESH,
        )

    def block(of, rep_half, k):
        return of * rows + rep_half * half + k * part

    def first(k):
        return remote(stage.at[pl.ds(rep * half + k * part, part), :], block(dp, rep, k), part, k, across)

    def whole():
        return remote(stage, dp * rows, rows, 4 * CHUNKS, partner)

    def place():
        return pltpu.make_async_copy(stage, out.at[pl.ds(dp * rows, rows), :], own.at[0])

    theirs = dp + 2 - 4 * x

    def onward(k, rep_half, n, device):
        at = block(theirs, rep_half, k)
        return remote(out.at[pl.ds(at, part), :], at, part, n * CHUNKS + k, device)

    def start():
        for copy in local():
            copy.start()
        barrier = pltpu.get_barrier_semaphore()
        for device in (across, group, partner):
            pl.semaphore_signal(barrier, inc=1, device_id=device, device_id_type=pl.DeviceIdType.MESH)
        pl.semaphore_wait(barrier, 3)
        for copy in local():
            copy.wait()
        for k in range(CHUNKS):
            first(k).start()
        whole().start()
        place().start()

    def relay(k):
        first(k).wait_recv()
        onward(k, rep, 1, group).start()
        onward(k, rep, 2, partner).start()

    def relay_other(k):
        onward(k, rep, 1, group).wait_recv()
        onward(k, 1 - rep, 3, partner).start()

    def finish():
        place().wait()
        whole().wait()
        for k in range(CHUNKS):
            first(k).wait_send()
            onward(k, rep, 1, group).wait_send()
            onward(k, rep, 2, partner).wait()
            onward(k, 1 - rep, 3, partner).wait()

    return start, relay, relay_other, finish


def _exchange_scratch(rows, columns):
    return [
        pltpu.VMEM((rows, columns), jnp.bfloat16),
        pltpu.SemaphoreType.DMA((7,)),
        pltpu.SemaphoreType.DMA((1,)),
        pltpu.SemaphoreType.DMA((4 * CHUNKS + 1,)),
        pltpu.SemaphoreType.DMA((4 * CHUNKS + 1,)),
    ]


def _fetch(wq, wk, wv, wo, out, stage, *sems, layer):
    start, relay, relay_other, finish = _exchange((wq, wk, wv, wo), out, stage, sems, layer=layer)
    start()
    relay(0)
    for k in range(1, CHUNKS):
        relay(k)
        relay_other(k - 1)
    relay_other(CHUNKS - 1)
    finish()


def fetch(wq, wk, wv, wo, layer, devices):
    rows, columns = wq.shape[1], 3 * wq.shape[2] + wo.shape[2]
    return pl.pallas_call(
        lambda *refs: _fetch(*refs, layer=layer),
        in_specs=[pl.BlockSpec(memory_space=pl.ANY)] * 4,
        out_specs=pl.BlockSpec(memory_space=pl.ANY),
        out_shape=jax.ShapeDtypeStruct((devices * rows, columns), jnp.bfloat16),
        scratch_shapes=_exchange_scratch(rows, columns),
        compiler_params=pltpu.CompilerParams(collective_id=layer, has_side_effects=True),
        cost_estimate=pl.CostEstimate(flops=20 * 10**9, transcendentals=0, bytes_accessed=2 * devices * rows * columns),
        name="fetch",
    )(wq, wk, wv, wo)


def _up_and_fetch(b_ref, wg_ref, wu_ref, wq, wk, wv, wo, gate_ref, up_ref, act_ref, out, stage, *sems, rows, layer):
    j, last = pl.program_id(0), pl.num_programs(0) - 1
    start, relay, relay_other, finish = _exchange((wq, wk, wv, wo), out, stage, sems, layer=layer)
    pl.when(j == 0)(start)
    for k in range(CHUNKS):
        pl.when(j == 3 + 3 * k)(lambda k=k: relay(k))
        pl.when(j == 5 + 3 * k)(lambda k=k: relay_other(k))
    _up(b_ref, wg_ref, wu_ref, gate_ref, up_ref, act_ref, rows=rows)
    pl.when(j == last)(finish)


def ffn_up_and_fetch(b, w_gate, w_up, wq, wk, wv, wo, layer, tile=256, rows=512):
    (tokens, d), ff = b.shape, w_gate.shape[1]
    own, columns = wq.shape[1], 3 * wq.shape[2] + wo.shape[2]
    weight = pl.BlockSpec((d, tile), lambda j: (0, j))
    out = pl.BlockSpec((tokens, tile), lambda j: (0, j))
    anywhere = pl.BlockSpec(memory_space=pl.ANY)
    return pl.pallas_call(
        lambda *refs: _up_and_fetch(*refs, rows=rows, layer=layer),
        grid=(ff // tile,),
        in_specs=[pl.BlockSpec((tokens, d), lambda j: (0, 0)), weight, weight] + [anywhere] * 4,
        out_specs=[out, out, out, anywhere],
        out_shape=[jax.ShapeDtypeStruct((tokens, ff), t) for t in (jnp.float32, jnp.float32, jnp.bfloat16)]
        + [jax.ShapeDtypeStruct((d, columns), jnp.bfloat16)],
        scratch_shapes=_exchange_scratch(own, columns),
        compiler_params=pltpu.CompilerParams(
            dimension_semantics=("arbitrary",), vmem_limit_bytes=VMEM, collective_id=layer, has_side_effects=True
        ),
        cost_estimate=pl.CostEstimate(flops=4 * tokens * d * ff, transcendentals=tokens * ff, bytes_accessed=10 * tokens * ff + 4 * d * ff),
        name="ffn_up_and_fetch",
    )(b, w_gate, w_up, wq, wk, wv, wo)


def parted(t):
    wide = GROUP * HEAD
    return [jnp.concatenate([t[:, a : a + wide] for a in range(n * wide, t.shape[1], 3 * wide)], axis=1) for n in range(3)]


def together(first, *rest):
    return lax.optimization_barrier((first, *rest))


def solution(mesh):
    reps = mesh.shape["rep"]

    def step(x, dy, *weights):
        layers = weights[0].shape[0]
        rep = lax.axis_index("rep")
        cos, sin = tables(x.shape[1])

        def mine(w, number):
            part = w.shape[1] // reps
            return lax.dynamic_slice(w, (number, rep * part, 0), (1, part, w.shape[2]))[0]

        def whole(shard):
            return lax.all_gather(shard, ("dp", "rep"), axis=0, tiled=True)

        def scatter(term):
            return lax.psum_scatter(term, "dp", scatter_dimension=0, tiled=True)

        fetched = []
        for n in range(layers):
            fetched.append([whole(mine(w, n)) for w in weights[4:]])
        three = 3 * weights[0].shape[2]

        h, kept = x[0], []
        square = fetch(*weights[:4], 0, mesh.shape["dp"])
        for n in range(layers):
            wg, wu, wd = fetched[n]
            a = normed(h)
            qkv = matmul(a, square[:, :three])
            o, lse = attend(qkv, cos, sin)
            h1 = h + matmul(o, square[:, three:])
            b = normed(h1)
            held = square
            if n < layers - 1:
                gate, up, act, square = ffn_up_and_fetch(b, wg, wu, *weights[:4], n + 1)
            else:
                gate, up, act = ffn_up(b, wg, wu)
            kept.append((h, a, qkv, o, lse, h1, b, gate, up, act, held))
            if n < layers - 1:
                h = h1 + matmul(act, wd)

        dh, grads, sums, out = dy[0], [None] * layers, {}, {}

        def after(value, *keys):
            for key in keys:
                if key in sums:
                    value, out[key] = together(value, sums.pop(key))
            return value

        for n in reversed(range(layers)):
            wg, wu, wd = fetched[n]
            h, a, qkv, o, lse, h1, b, gate, up, act, square = kept[n]
            d_down = matmul_tn(act, dh)
            dh, d_down = together(dh, d_down)
            sums["down", n] = scatter(d_down)
            dg, du = ffn_down_bwd(dh, wd, gate, up)
            dg = after(dg, ("qkv", n + 1))
            d_gate = matmul_tn(b, dg)
            sums["gate", n] = scatter(d_gate)
            dg, du, d_gate = together(dg, du, d_gate)
            du = after(du, ("down", n))
            d_up = matmul_tn(b, du)
            dg, du, d_up = together(dg, du, d_up)
            sums["up", n] = scatter(d_up)
            db = matmul_nt(dg, wg) + matmul_nt(du, wu)
            dh1 = after(normed_bwd(h1, db, dh), ("gate", n))
            d_o = matmul_tn(o, dh1)
            dh1, d_o = together(dh1, d_o)
            sums["o", n] = scatter(d_o)
            do = matmul_nt(dh1, square[:, three:])
            dqkv = after(attend_bwd(qkv, o, do, lse, cos, sin), ("up", n))
            d_qkv = matmul_tn(a, dqkv)
            dqkv, d_qkv = together(dqkv, d_qkv)
            dqkv = after(dqkv, ("o", n))
            sums["qkv", n] = scatter(d_qkv)
            dh = normed_bwd(h, matmul_nt(dqkv, square[:, :three]), dh1)
        out |= sums
        grads = [(*parted(out["qkv", n]), *(out[name, n] for name in ("o", "gate", "up", "down"))) for n in range(layers)]
        return (dh[None], *(jnp.stack([g[i] for g in grads]) for i in range(7)))

    states, cut = P(("rep", "dp"), None, None), P(None, "dp", None)
    return jax.shard_map(
        step,
        mesh=mesh,
        in_specs=(states, states) + (cut,) * 7,
        out_specs=(states,) + (P("rep", "dp", None),) * 7,
        check_vma=False,
    )
```

```python
import jax
import jax.numpy as jnp
from jax import lax
from jax.experimental import pallas as pl
from jax.experimental.pallas import tpu as pltpu
from jax.sharding import PartitionSpec as P

HEAD = 128
THETA = 10000
EPS = 1e-6
NEG = -1e30
LOG2E = 1.4426950408889634
VMEM = 60 * 2**20
GROUP = 4
BLOCK = 512


def _dot(a, b, ca, cb):
    return lax.dot_general(a, b, (((ca,), (cb,)), ((), ())), preferred_element_type=jnp.float32)


def _turn(t, cos, sin):
    return t * cos + pltpu.roll(t, HEAD // 2, 1) * sin


def _turn_back(t, cos, sin):
    return t * cos + pltpu.roll(t * sin, HEAD // 2, 1)


def _hide(s, first_query, first_key):
    query = lax.broadcasted_iota(jnp.int32, s.shape, 1) + first_query
    key = lax.broadcasted_iota(jnp.int32, s.shape, 0) + first_key
    return query >= key


def _attend(q_ref, k_ref, v_ref, cos_ref, sin_ref, o_ref, lse_ref, qr, kr, top_s, mix_s, *, scale):
    iq = pl.program_id(1)
    e = scale * LOG2E
    rows = pl.ds(pl.multiple_of(iq * BLOCK, BLOCK), BLOCK)
    cos, sin = cos_ref[rows, :], sin_ref[rows, :]
    for i in range(GROUP):
        at = slice(i * HEAD, (i + 1) * HEAD)
        kr[rows, at] = _turn(k_ref[rows, at].astype(jnp.float32), cos, sin).astype(jnp.bfloat16)
        qr[:, at] = _turn(q_ref[:, at].astype(jnp.float32), cos, sin).astype(jnp.bfloat16)
    top_s[...] = jnp.full(top_s.shape, NEG, jnp.float32)
    mix_s[...] = jnp.zeros(mix_s.shape, jnp.float32)

    def block(first_key, keys, first_query, masked):
        here = pl.ds(first_key, keys)
        ones = jnp.ones((8, keys), jnp.bfloat16)
        cols = slice(first_query, BLOCK)
        scores = [_dot(kr[here, i * HEAD : (i + 1) * HEAD], qr[cols, i * HEAD : (i + 1) * HEAD], 1, 1) for i in range(GROUP)]
        ok = _hide(scores[0], 0, 0) if masked else None
        weights, keeps = [], []
        for i, s in enumerate(scores):
            if masked:
                s = jnp.where(ok, s, 2 * NEG)
            old = top_s[i : i + 1, cols]
            top = jnp.maximum(old, s.max(axis=0, keepdims=True))
            top_s[i : i + 1, cols] = top
            weights.append(jnp.exp2((s - top) * e).astype(jnp.bfloat16))
            keeps.append(jnp.exp2((old - top) * e))
        for i, (p, keep) in enumerate(zip(weights, keeps)):
            values = jnp.concatenate([v_ref[here, i * HEAD : (i + 1) * HEAD].T, ones], axis=0)
            mix_s[i, :, cols] = mix_s[i, :, cols] * keep + _dot(values, p, 1, 0)

    lax.fori_loop(0, iq, lambda j, _: block(pl.multiple_of(j * BLOCK, BLOCK), BLOCK, 0, False), None)
    for n in range(0, BLOCK, 256):
        block(pl.multiple_of(iq * BLOCK + n, 256), 256, n, True)
    for i in range(GROUP):
        total = mix_s[i, HEAD : HEAD + 1, :]
        o_ref[:, i * HEAD : (i + 1) * HEAD] = (mix_s[i, :HEAD, :] * (1 / total)).T.astype(jnp.bfloat16)
        lse_ref[0, i : i + 1, :] = top_s[i : i + 1, :] * scale + jnp.log(total)


def attend(qkv, cos, sin):
    tokens, wide = qkv.shape[0], GROUP * HEAD
    groups = qkv.shape[1] // (3 * wide)
    table = pl.BlockSpec((tokens, HEAD), lambda g, i: (0, 0))
    return pl.pallas_call(
        lambda *refs: _attend(*refs, scale=HEAD**-0.5),
        grid=(groups, tokens // BLOCK),
        in_specs=[
            pl.BlockSpec((BLOCK, wide), lambda g, i: (i, 3 * g)),
            pl.BlockSpec((tokens, wide), lambda g, i: (0, 3 * g + 1)),
            pl.BlockSpec((tokens, wide), lambda g, i: (0, 3 * g + 2)),
            table,
            table,
        ],
        out_specs=[pl.BlockSpec((BLOCK, wide), lambda g, i: (i, g)), pl.BlockSpec((1, GROUP, BLOCK), lambda g, i: (g, 0, i))],
        out_shape=[
            jax.ShapeDtypeStruct((tokens, groups * wide), jnp.bfloat16),
            jax.ShapeDtypeStruct((groups, GROUP, tokens), jnp.float32),
        ],
        scratch_shapes=[
            pltpu.VMEM((BLOCK, wide), jnp.bfloat16),
            pltpu.VMEM((tokens, wide), jnp.bfloat16),
            pltpu.VMEM((8, BLOCK), jnp.float32),
            pltpu.VMEM((GROUP, HEAD + 8, BLOCK), jnp.float32),
        ],
        compiler_params=pltpu.CompilerParams(dimension_semantics=("arbitrary", "arbitrary"), vmem_limit_bytes=VMEM),
        cost_estimate=pl.CostEstimate(flops=30 * 10**9, transcendentals=20 * 10**6, bytes_accessed=20 * 2**20),
        name="attend",
    )(qkv, qkv, qkv, cos, sin)


def _attend_bwd(q_ref, k_ref, v_ref, o_ref, do_ref, lse_ref, cos_ref, sin_ref, d_ref, qr, kr, dq_s, dk_s, dv_s, *, scale):
    iq, last = pl.program_id(1), pl.num_programs(1) - 1
    e = scale * LOG2E
    wide = GROUP * HEAD
    rows = pl.ds(pl.multiple_of(iq * BLOCK, BLOCK), BLOCK)
    cos, sin = cos_ref[rows, :], sin_ref[rows, :]
    lses, deltas = [], []
    for i in range(GROUP):
        at = slice(i * HEAD, (i + 1) * HEAD)
        kr[rows, at] = _turn(k_ref[rows, at].astype(jnp.float32), cos, sin).astype(jnp.bfloat16)
        qr[:, at] = _turn(q_ref[:, at].astype(jnp.float32), cos, sin).astype(jnp.bfloat16)
        lses.append(lse_ref[0, i : i + 1, :] * LOG2E)
        deltas.append((do_ref[:, at].astype(jnp.float32) * o_ref[:, at].astype(jnp.float32)).T.sum(axis=0, keepdims=True))
    dq_s[...] = jnp.zeros(dq_s.shape, jnp.float32)
    dk_s[rows, :] = jnp.zeros((BLOCK, wide), jnp.float32)
    dv_s[rows, :] = jnp.zeros((BLOCK, wide), jnp.float32)

    def block(first_key, keys, first_query, masked):
        here = pl.ds(first_key, keys)
        cols = slice(first_query, BLOCK)
        heads = [slice(i * HEAD, (i + 1) * HEAD) for i in range(GROUP)]
        scores = [_dot(kr[here, at], qr[cols, at], 1, 1) for at in heads]
        dps = [_dot(v_ref[here, at], do_ref[cols, at], 1, 1) for at in heads]
        ok = _hide(scores[0], 0, 0) if masked else None
        for i, at in enumerate(heads):
            p = jnp.exp2(scores[i] * e - lses[i][:, cols])
            if masked:
                p = jnp.where(ok, p, 0.0)
            ds = (p * (dps[i] - deltas[i][:, cols])).astype(jnp.bfloat16)
            dv_s[here, at] += _dot(p.astype(jnp.bfloat16), do_ref[cols, at], 1, 0)
            dk_s[here, at] += _dot(ds, qr[cols, at], 1, 0)
            dq_s[i, :, cols] += _dot(kr[here, at].T, ds, 1, 0)

    lax.fori_loop(0, iq, lambda j, _: block(pl.multiple_of(j * BLOCK, BLOCK), BLOCK, 0, False), None)
    for n in range(0, BLOCK, 256):
        block(pl.multiple_of(iq * BLOCK + n, 256), 256, n, True)

    def narrow(t):
        return t.astype(jnp.bfloat16).astype(jnp.float32)

    for i in range(GROUP):
        at = slice(i * HEAD, (i + 1) * HEAD)
        d_ref[rows, at] = _turn_back(narrow((dq_s[i] * scale).T), cos, sin).astype(jnp.bfloat16)

    @pl.when(iq == last)
    def _():
        def finish(n, _):
            here = pl.ds(pl.multiple_of(n * BLOCK, BLOCK), BLOCK)
            c, s = cos_ref[here, :], sin_ref[here, :]
            for i in range(GROUP):
                at = slice(i * HEAD, (i + 1) * HEAD)
                d_ref[here, wide + i * HEAD : wide + (i + 1) * HEAD] = _turn_back(narrow(dk_s[here, at] * scale), c, s).astype(jnp.bfloat16)
            d_ref[here, 2 * wide :] = dv_s[here, :].astype(jnp.bfloat16)

        lax.fori_loop(0, last + 1, finish, None)


def attend_bwd(qkv, o, do, lse, cos, sin):
    tokens, wide = qkv.shape[0], GROUP * HEAD
    groups = qkv.shape[1] // (3 * wide)
    table = pl.BlockSpec((tokens, HEAD), lambda g, i: (0, 0))
    own = pl.BlockSpec((BLOCK, wide), lambda g, i: (i, g))
    return pl.pallas_call(
        lambda *refs: _attend_bwd(*refs, scale=HEAD**-0.5),
        grid=(groups, tokens // BLOCK),
        in_specs=[
            pl.BlockSpec((BLOCK, wide), lambda g, i: (i, 3 * g)),
            pl.BlockSpec((tokens, wide), lambda g, i: (0, 3 * g + 1)),
            pl.BlockSpec((tokens, wide), lambda g, i: (0, 3 * g + 2)),
            own,
            own,
            pl.BlockSpec((1, GROUP, BLOCK), lambda g, i: (g, 0, i)),
            table,
            table,
        ],
        out_specs=pl.BlockSpec((tokens, 3 * wide), lambda g, i: (0, g)),
        out_shape=jax.ShapeDtypeStruct((tokens, groups * 3 * wide), jnp.bfloat16),
        scratch_shapes=[
            pltpu.VMEM((BLOCK, wide), jnp.bfloat16),
            pltpu.VMEM((tokens, wide), jnp.bfloat16),
            pltpu.VMEM((GROUP, HEAD, BLOCK), jnp.float32),
            pltpu.VMEM((tokens, wide), jnp.float32),
            pltpu.VMEM((tokens, wide), jnp.float32),
        ],
        compiler_params=pltpu.CompilerParams(dimension_semantics=("arbitrary", "arbitrary"), vmem_limit_bytes=VMEM),
        cost_estimate=pl.CostEstimate(flops=groups * 30 * 10**9, transcendentals=groups * 10**7, bytes_accessed=groups * 20 * 2**20),
        name="attend_bwd",
    )(qkv, qkv, qkv, o, do, lse, cos, sin)


def _up(b_ref, wg_ref, wu_ref, gate_ref, up_ref, act_ref):
    rows = gate_ref.shape[0]
    b = b_ref[pl.ds(pl.multiple_of(pl.program_id(1) * rows, rows), rows), :]
    gate, up = _dot(b, wg_ref[...], 1, 0), _dot(b, wu_ref[...], 1, 0)
    gate_ref[...] = gate
    up_ref[...] = up
    act_ref[...] = (gate * jax.nn.sigmoid(gate) * up).astype(jnp.bfloat16)


UP = (2048, 256)
TILE = 256
CUT = 512


def _up_parts(b, w_gate):
    (tokens, d), ff = b.shape, w_gate.shape[1]
    rows, tile = UP
    weight = pl.BlockSpec((d, tile), lambda j, i: (0, j))
    out = pl.BlockSpec((rows, tile), lambda j, i: (i, j))
    shapes = [jax.ShapeDtypeStruct((tokens, ff), t) for t in (jnp.float32, jnp.float32, jnp.bfloat16)]
    return (ff // tile, tokens // rows), [pl.BlockSpec((tokens, d), lambda j, i: (0, 0)), weight, weight], [out] * 3, shapes


def _up_cost(b, w_gate):
    (tokens, d), ff = b.shape, w_gate.shape[1]
    return pl.CostEstimate(flops=4 * tokens * d * ff, transcendentals=tokens * ff, bytes_accessed=10 * tokens * ff + 4 * d * ff)


def ffn_up(b, w_gate, w_up):
    grid, ins, outs, shapes = _up_parts(b, w_gate)
    return pl.pallas_call(
        _up,
        grid=grid,
        in_specs=ins,
        out_specs=outs,
        out_shape=shapes,
        compiler_params=pltpu.CompilerParams(dimension_semantics=("arbitrary",) * 2, vmem_limit_bytes=VMEM),
        cost_estimate=_up_cost(b, w_gate),
        name="ffn_up",
    )(b, w_gate, w_up)


def _ffn_bwd(dh_ref, wd_ref, gate_ref, up_ref, b_ref, dg_ref, du_ref, wg_ref, wu_ref, turned):
    @pl.when(pl.program_id(0) == 0)
    def _():
        for at in range(0, b_ref.shape[0], CUT):
            turned[:, at : at + CUT] = b_ref[at : at + CUT, :].T

    for at in range(0, dh_ref.shape[0], CUT):
        here = slice(at, at + CUT)
        dact = _dot(dh_ref[here, :], wd_ref[...], 1, 1).astype(jnp.bfloat16).astype(jnp.float32)
        gate, up = gate_ref[here, :], up_ref[here, :]
        s = jax.nn.sigmoid(gate)
        silu = gate * s
        du_ref[here, :] = (dact * silu).astype(jnp.bfloat16)
        dg_ref[here, :] = (dact * up * (s + silu * (1 - s))).astype(jnp.bfloat16)
    wg_ref[...] = _dot(turned[...], dg_ref[...], 1, 0).astype(jnp.bfloat16)
    wu_ref[...] = _dot(turned[...], du_ref[...], 1, 0).astype(jnp.bfloat16)


def _ffn_bwd_and_sum(dh_ref, wd_ref, gate_ref, up_ref, b_ref, term, dg_ref, du_ref, wg_ref, wu_ref, out, turned, *scratch):
    run = _reduction(term, out, *scratch)
    run(pl.program_id(0), pl.num_programs(0), lambda: _ffn_bwd(dh_ref, wd_ref, gate_ref, up_ref, b_ref, dg_ref, du_ref, wg_ref, wu_ref, turned))


def ffn_bwd(dh, w_down, gate, up, b, term=None, devices=None, number=None):
    (tokens, d), ff = dh.shape, w_down.shape[0]
    held = pl.BlockSpec((tokens, d), lambda j: (0, 0))
    cut, grad = pl.BlockSpec((tokens, TILE), lambda j: (0, j)), pl.BlockSpec((d, TILE), lambda j: (0, j))
    ins, outs = [held, pl.BlockSpec((TILE, d), lambda j: (j, 0)), cut, cut, held], [cut, cut, grad, grad]
    shapes = [jax.ShapeDtypeStruct((tokens, ff), jnp.bfloat16)] * 2 + [jax.ShapeDtypeStruct((d, ff), jnp.bfloat16)] * 2
    scratch, more, given = [pltpu.VMEM((d, tokens), jnp.bfloat16)], {}, [dh, w_down, gate, up, b]
    if term is not None:
        block = (term.shape[0] // devices, term.shape[1])
        ins, outs = ins + [pl.BlockSpec(memory_space=pl.ANY)], outs + [pl.BlockSpec(memory_space=pl.ANY)]
        shapes, scratch = shapes + [jax.ShapeDtypeStruct(block, jnp.bfloat16)], scratch + _reduction_scratch(*block)
        more, given = {"collective_id": number, "has_side_effects": True}, given + [term]
    return pl.pallas_call(
        _ffn_bwd if term is None else _ffn_bwd_and_sum,
        grid=(ff // TILE,),
        in_specs=ins,
        out_specs=outs,
        out_shape=shapes,
        scratch_shapes=scratch,
        compiler_params=pltpu.CompilerParams(dimension_semantics=("arbitrary",), vmem_limit_bytes=VMEM, **more),
        cost_estimate=pl.CostEstimate(flops=6 * tokens * d * ff, transcendentals=tokens * ff, bytes_accessed=12 * tokens * ff + 6 * d * ff),
        name="ffn_bwd",
    )(*given)


def matmul(a, w):
    return jnp.dot(a, w, preferred_element_type=jnp.float32).astype(jnp.bfloat16)


def matmul_nt(a, w):
    return _dot(a, w, 1, 1).astype(jnp.bfloat16)


def matmul_tn(a, b):
    return _dot(a, b, 0, 0).astype(jnp.bfloat16)


def norm_scale(h):
    return lax.rsqrt(jnp.mean(h.astype(jnp.float32) ** 2, -1, keepdims=True) + EPS)


def normed(h):
    return (h.astype(jnp.float32) * norm_scale(h)).astype(jnp.bfloat16)


def normed_bwd(h, da, dh):
    wide, da = h.astype(jnp.float32), da.astype(jnp.float32)
    scale = norm_scale(h)
    inner = jnp.sum(da * wide, -1, keepdims=True) * (scale**3 / h.shape[-1])
    return (dh.astype(jnp.float32) + (da * scale - wide * inner).astype(jnp.bfloat16).astype(jnp.float32)).astype(jnp.bfloat16)


def tables(tokens):
    half = HEAD // 2
    angle = jnp.arange(tokens, dtype=jnp.float32)[:, None] * THETA ** (-jnp.arange(half, dtype=jnp.float32) / half)
    cos, sin = jnp.cos(angle), jnp.sin(angle)
    return jnp.concatenate([cos, cos], -1), jnp.concatenate([-sin, sin], -1)


CHUNKS = 4


def _exchange(refs, out, stage, sems, *, layer):
    loaded, own, sends, recvs = sems
    rep, dp = lax.axis_index("rep"), lax.axis_index("dp")
    x, core = dp // 2, dp % 2
    across = (rep, dp + 2 - 4 * x)
    group = (1 - rep, dp)
    partner = (rep, dp + 1 - 2 * core)
    rows = refs[0].shape[1]
    half = rows // 2
    part = half // CHUNKS
    wide = GROUP * HEAD
    square = refs[0].shape[2]

    def local():
        copies = []
        for a in range(0, square, wide):
            for i in range(3):
                copies.append((refs[i].at[layer, :, pl.ds(a, wide)], stage.at[:, pl.ds(3 * a + i * wide, wide)]))
        copies.append((refs[3].at[layer], stage.at[:, pl.ds(3 * square, refs[3].shape[2])]))
        return [pltpu.make_async_copy(s, d, loaded.at[n]) for n, (s, d) in enumerate(copies)]

    def remote(source, at, size, n, device):
        return pltpu.make_async_remote_copy(
            src_ref=source, dst_ref=out.at[pl.ds(at, size), :], send_sem=sends.at[n], recv_sem=recvs.at[n],
            device_id=device, device_id_type=pl.DeviceIdType.MESH,
        )

    def block(of, rep_half, k):
        return of * rows + rep_half * half + k * part

    def first(k):
        return remote(stage.at[pl.ds(rep * half + k * part, part), :], block(dp, rep, k), part, k, across)

    def whole():
        return remote(stage, dp * rows, rows, 4 * CHUNKS, partner)

    def place():
        return pltpu.make_async_copy(stage, out.at[pl.ds(dp * rows, rows), :], own.at[0])

    theirs = dp + 2 - 4 * x

    def onward(k, rep_half, n, device):
        at = block(theirs, rep_half, k)
        return remote(out.at[pl.ds(at, part), :], at, part, n * CHUNKS + k, device)

    def start():
        for copy in local():
            copy.start()
        barrier = pltpu.get_barrier_semaphore()
        for device in (across, group, partner):
            pl.semaphore_signal(barrier, inc=1, device_id=device, device_id_type=pl.DeviceIdType.MESH)
        pl.semaphore_wait(barrier, 3)
        for copy in local():
            copy.wait()
        for k in range(CHUNKS):
            first(k).start()
        whole().start()
        place().start()

    def relay(k):
        first(k).wait_recv()
        onward(k, rep, 1, group).start()
        onward(k, rep, 2, partner).start()

    def relay_other(k):
        onward(k, rep, 1, group).wait_recv()
        onward(k, 1 - rep, 3, partner).start()

    def finish():
        place().wait()
        whole().wait()
        for k in range(CHUNKS):
            first(k).wait_send()
            onward(k, rep, 1, group).wait_send()
            onward(k, rep, 2, partner).wait()
            onward(k, 1 - rep, 3, partner).wait()

    return start, relay, relay_other, finish


def _exchange_scratch(rows, columns):
    return [
        pltpu.VMEM((rows, columns), jnp.bfloat16),
        pltpu.SemaphoreType.DMA((7,)),
        pltpu.SemaphoreType.DMA((1,)),
        pltpu.SemaphoreType.DMA((4 * CHUNKS + 1,)),
        pltpu.SemaphoreType.DMA((4 * CHUNKS + 1,)),
    ]


def _fetch(wq, wk, wv, wo, out, stage, *sems, layer):
    start, relay, relay_other, finish = _exchange((wq, wk, wv, wo), out, stage, sems, layer=layer)
    start()
    relay(0)
    for k in range(1, CHUNKS):
        relay(k)
        relay_other(k - 1)
    relay_other(CHUNKS - 1)
    finish()


def fetch(wq, wk, wv, wo, layer, devices):
    rows, columns = wq.shape[1], 3 * wq.shape[2] + wo.shape[2]
    return pl.pallas_call(
        lambda *refs: _fetch(*refs, layer=layer),
        in_specs=[pl.BlockSpec(memory_space=pl.ANY)] * 4,
        out_specs=pl.BlockSpec(memory_space=pl.ANY),
        out_shape=jax.ShapeDtypeStruct((devices * rows, columns), jnp.bfloat16),
        scratch_shapes=_exchange_scratch(rows, columns),
        compiler_params=pltpu.CompilerParams(collective_id=layer, has_side_effects=True),
        cost_estimate=pl.CostEstimate(flops=20 * 10**9, transcendentals=0, bytes_accessed=2 * devices * rows * columns),
        name="fetch",
    )(wq, wk, wv, wo)


def _up_and_fetch(b_ref, wg_ref, wu_ref, wq, wk, wv, wo, gate_ref, up_ref, act_ref, out, stage, *sems, layer):
    step, last = pl.program_id(0) * pl.num_programs(1) + pl.program_id(1), pl.num_programs(0) * pl.num_programs(1) - 1
    start, relay, relay_other, finish = _exchange((wq, wk, wv, wo), out, stage, sems, layer=layer)
    pl.when(step == 0)(start)
    for k in range(CHUNKS):
        pl.when(step == 3 + 3 * k)(lambda k=k: relay(k))
        pl.when(step == 5 + 3 * k)(lambda k=k: relay_other(k))
    _up(b_ref, wg_ref, wu_ref, gate_ref, up_ref, act_ref)
    pl.when(step == last)(finish)


def ffn_up_and_fetch(b, w_gate, w_up, wq, wk, wv, wo, layer):
    grid, ins, outs, shapes = _up_parts(b, w_gate)
    own, columns = wq.shape[1], 3 * wq.shape[2] + wo.shape[2]
    anywhere = pl.BlockSpec(memory_space=pl.ANY)
    return pl.pallas_call(
        lambda *refs: _up_and_fetch(*refs, layer=layer),
        grid=grid,
        in_specs=ins + [anywhere] * 4,
        out_specs=outs + [anywhere],
        out_shape=shapes + [jax.ShapeDtypeStruct((b.shape[1], columns), jnp.bfloat16)],
        scratch_shapes=_exchange_scratch(own, columns),
        compiler_params=pltpu.CompilerParams(
            dimension_semantics=("arbitrary",) * 2, vmem_limit_bytes=VMEM, collective_id=layer, has_side_effects=True
        ),
        cost_estimate=_up_cost(b, w_gate),
        name="ffn_up_and_fetch",
    )(b, w_gate, w_up, wq, wk, wv, wo)


PARTS = 4


def _reduction(term, out, mine, partners, total, theirs, loaded, sends, recvs):
    rows = out.shape[0]
    part = rows // PARTS
    rep, dp = lax.axis_index("rep"), lax.axis_index("dp")
    x, core = dp // 2, dp % 2
    across, partner = (rep, dp + 2 - 4 * x), (rep, dp + 1 - 2 * core)

    def remote(source, target, n, device):
        return pltpu.make_async_remote_copy(
            src_ref=source, dst_ref=target, send_sem=sends.at[n], recv_sem=recvs.at[n],
            device_id=device, device_id_type=pl.DeviceIdType.MESH,
        )

    def of(block, k):
        owner = (1 - x if block == 0 else x) * 2
        return owner * rows + k * part

    def here(k):
        return pl.ds(k * part, part)

    def load(block, k):
        return pltpu.make_async_copy(term.at[pl.ds(of(block, k) + core * rows, part), :], mine.at[block, here(k), :], loaded.at[block * PARTS + k])

    def give(block, k):
        source = term.at[pl.ds(of(block, k) + (1 - core) * rows, part), :]
        return remote(source, partners.at[block, here(k), :], block * PARTS + k, partner)

    def send(k):
        return remote(total.at[here(k), :], theirs.at[here(k), :], 2 * PARTS + k, across)

    def put(k):
        return pltpu.make_async_copy(mine.at[1, here(k), :], out.at[here(k), :], loaded.at[2 * PARTS + k])

    def start():
        barrier = pltpu.get_barrier_semaphore()
        for device in (across, partner):
            pl.semaphore_signal(barrier, inc=1, device_id=device, device_id_type=pl.DeviceIdType.MESH)
        for block in range(2):
            for k in range(PARTS):
                load(block, k).start()
        pl.semaphore_wait(barrier, 2)
        for block in range(2):
            for k in range(PARTS):
                give(block, k).start()

    def add(k):
        load(0, k).wait()
        give(0, k).wait_recv()
        total[here(k), :] = (mine[0, here(k), :].astype(jnp.float32) + partners[0, here(k), :].astype(jnp.float32)).astype(jnp.bfloat16)

    def close(k):
        load(1, k).wait()
        give(1, k).wait_recv()
        send(k).wait_recv()
        own = mine[1, here(k), :].astype(jnp.float32) + partners[1, here(k), :].astype(jnp.float32)
        mine[1, here(k), :] = (own + theirs[here(k), :].astype(jnp.float32)).astype(jnp.bfloat16)

    def finish():
        for k in range(PARTS):
            put(k).wait()
            send(k).wait_send()
            for block in range(2):
                give(block, k).wait_send()

    def run(step, steps, body):
        pl.when(step == 0)(start)
        for k in range(PARTS):
            pl.when(step == 1 + k)(lambda k=k: add(k))
            pl.when(step == 2 + k)(lambda k=k: send(k).start())
        for k in range(PARTS - 1):
            at = steps - 8 + 3 * k
            pl.when(step == at)(lambda k=k: close(k))
            pl.when(step == at + 1)(lambda k=k: put(k).start())
        body()

        @pl.when(step == steps - 1)
        def _():
            close(PARTS - 1)
            put(PARTS - 1).start()
            finish()

    return run


def _reduction_scratch(rows, columns):
    return [
        pltpu.VMEM((2, rows, columns), jnp.bfloat16),
        pltpu.VMEM((2, rows, columns), jnp.bfloat16),
        pltpu.VMEM((rows, columns), jnp.bfloat16),
        pltpu.VMEM((rows, columns), jnp.bfloat16),
        pltpu.SemaphoreType.DMA((3 * PARTS,)),
        pltpu.SemaphoreType.DMA((3 * PARTS,)),
        pltpu.SemaphoreType.DMA((3 * PARTS,)),
    ]


def parted(t):
    wide = GROUP * HEAD
    return [jnp.concatenate([t[:, a : a + wide] for a in range(n * wide, t.shape[1], 3 * wide)], axis=1) for n in range(3)]


def together(first, *rest):
    return lax.optimization_barrier((first, *rest))


def solution(mesh):
    reps = mesh.shape["rep"]

    def step(x, dy, *weights):
        layers = weights[0].shape[0]
        rep = lax.axis_index("rep")
        cos, sin = tables(x.shape[1])

        def mine(w, number):
            part = w.shape[1] // reps
            return lax.dynamic_slice(w, (number, rep * part, 0), (1, part, w.shape[2]))[0]

        def whole(shard):
            return lax.all_gather(shard, ("dp", "rep"), axis=0, tiled=True)

        def scatter(term):
            return lax.psum_scatter(term, "dp", scatter_dimension=0, tiled=True)

        fetched = []
        for n in range(layers):
            fetched.append([whole(mine(w, n)) for w in weights[4:]])
        three = 3 * weights[0].shape[2]

        h, kept = x[0], []
        square = fetch(*weights[:4], 0, mesh.shape["dp"])
        for n in range(layers):
            wg, wu, wd = fetched[n]
            a = normed(h)
            qkv = matmul(a, square[:, :three])
            o, lse = attend(qkv, cos, sin)
            h1 = h + matmul(o, square[:, three:])
            b = normed(h1)
            held = square
            if n < layers - 1:
                gate, up, act, square = ffn_up_and_fetch(b, wg, wu, *weights[:4], n + 1)
            else:
                gate, up, act = ffn_up(b, wg, wu)
            kept.append((h, a, qkv, o, lse, h1, b, gate, up, act, held))
            if n < layers - 1:
                h = h1 + matmul(act, wd)

        dh, grads, sums, out = dy[0], [None] * layers, {}, {}

        def after(value, *keys):
            for key in keys:
                if key in sums:
                    value, out[key] = together(value, sums.pop(key))
            return value

        for n in reversed(range(layers)):
            wg, wu, wd = fetched[n]
            h, a, qkv, o, lse, h1, b, gate, up, act, square = kept[n]
            dh = after(dh, ("up", n + 1))
            d_down = matmul_tn(act, dh)
            dh, d_down = together(dh, d_down)
            dg, du, d_gate, d_up, out["down", n] = ffn_bwd(dh, wd, gate, up, b, d_down, mesh.shape["dp"], layers + n)
            dg = after(dg, ("o", n + 1), ("qkv", n + 1))
            sums["gate", n], sums["up", n] = scatter(d_gate), scatter(d_up)
            db = matmul_nt(dg, wg) + matmul_nt(du, wu)
            dh1 = normed_bwd(h1, db, dh)
            d_o = matmul_tn(o, dh1)
            dh1, d_o = together(dh1, d_o)
            sums["o", n] = scatter(d_o)
            do = matmul_nt(dh1, square[:, three:])
            dqkv = after(attend_bwd(qkv, o, do, lse, cos, sin), ("gate", n))
            d_qkv = matmul_tn(a, dqkv)
            dqkv, d_qkv = together(dqkv, d_qkv)
            sums["qkv", n] = scatter(d_qkv)
            da = matmul_nt(dqkv, square[:, :three])
            dh = normed_bwd(h, da, dh1)
        out |= sums
        grads = []
        for n in range(layers):
            grads.append((*parted(out["qkv", n]), *(out[name, n] for name in ("o", "gate", "up", "down"))))
        return (dh[None], *(jnp.stack([g[i] for g in grads]) for i in range(7)))

    states, cut = P(("rep", "dp"), None, None), P(None, "dp", None)
    return jax.shard_map(
        step,
        mesh=mesh,
        in_specs=(states, states) + (cut,) * 7,
        out_specs=(states,) + (P("rep", "dp", None),) * 7,
        check_vma=False,
    )
```

```python
import jax
import jax.numpy as jnp
from jax import lax
from jax.experimental import pallas as pl
from jax.experimental.pallas import tpu as pltpu
from jax.sharding import PartitionSpec as P

HEAD = 128
THETA = 10000
EPS = 1e-6
NEG = -1e30
LOG2E = 1.4426950408889634
VMEM = 60 * 2**20
GROUP = 4
BLOCK = 512


def _dot(a, b, ca, cb):
    return lax.dot_general(a, b, (((ca,), (cb,)), ((), ())), preferred_element_type=jnp.float32)


def _turn(t, cos, sin):
    return t * cos + pltpu.roll(t, HEAD // 2, 1) * sin


def _turn_back(t, cos, sin):
    return t * cos + pltpu.roll(t * sin, HEAD // 2, 1)


def _hide(s, first_query, first_key):
    query = lax.broadcasted_iota(jnp.int32, s.shape, 1) + first_query
    key = lax.broadcasted_iota(jnp.int32, s.shape, 0) + first_key
    return query >= key


def _attend(q_ref, k_ref, v_ref, cos_ref, sin_ref, o_ref, lse_ref, qr, kr, top_s, mix_s, *, scale):
    iq = pl.program_id(1)
    e = scale * LOG2E
    rows = pl.ds(pl.multiple_of(iq * BLOCK, BLOCK), BLOCK)
    cos, sin = cos_ref[rows, :], sin_ref[rows, :]
    for i in range(GROUP):
        at = slice(i * HEAD, (i + 1) * HEAD)
        kr[rows, at] = _turn(k_ref[rows, at].astype(jnp.float32), cos, sin).astype(jnp.bfloat16)
        qr[:, at] = _turn(q_ref[:, at].astype(jnp.float32), cos, sin).astype(jnp.bfloat16)
    top_s[...] = jnp.full(top_s.shape, NEG, jnp.float32)
    mix_s[...] = jnp.zeros(mix_s.shape, jnp.float32)

    def block(first_key, keys, first_query, masked):
        here = pl.ds(first_key, keys)
        ones = jnp.ones((8, keys), jnp.bfloat16)
        cols = slice(first_query, BLOCK)
        scores = [_dot(kr[here, i * HEAD : (i + 1) * HEAD], qr[cols, i * HEAD : (i + 1) * HEAD], 1, 1) for i in range(GROUP)]
        ok = _hide(scores[0], 0, 0) if masked else None
        weights, keeps = [], []
        for i, s in enumerate(scores):
            if masked:
                s = jnp.where(ok, s, 2 * NEG)
            old = top_s[i : i + 1, cols]
            top = jnp.maximum(old, s.max(axis=0, keepdims=True))
            top_s[i : i + 1, cols] = top
            weights.append(jnp.exp2((s - top) * e).astype(jnp.bfloat16))
            keeps.append(jnp.exp2((old - top) * e))
        for i, (p, keep) in enumerate(zip(weights, keeps)):
            values = jnp.concatenate([v_ref[here, i * HEAD : (i + 1) * HEAD].T, ones], axis=0)
            mix_s[i, :, cols] = mix_s[i, :, cols] * keep + _dot(values, p, 1, 0)

    lax.fori_loop(0, iq, lambda j, _: block(pl.multiple_of(j * BLOCK, BLOCK), BLOCK, 0, False), None)
    for n in range(0, BLOCK, 256):
        block(pl.multiple_of(iq * BLOCK + n, 256), 256, n, True)
    for i in range(GROUP):
        total = mix_s[i, HEAD : HEAD + 1, :]
        o_ref[:, i * HEAD : (i + 1) * HEAD] = (mix_s[i, :HEAD, :] * (1 / total)).T.astype(jnp.bfloat16)
        lse_ref[0, i : i + 1, :] = top_s[i : i + 1, :] * scale + jnp.log(total)


def _attend_bwd(q_ref, k_ref, v_ref, o_ref, do_ref, lse_ref, cos_ref, sin_ref, d_ref, qr, kr, dq_s, dk_s, dv_s, *, scale):
    iq, last = pl.program_id(1), pl.num_programs(1) - 1
    e = scale * LOG2E
    wide = GROUP * HEAD
    rows = pl.ds(pl.multiple_of(iq * BLOCK, BLOCK), BLOCK)
    cos, sin = cos_ref[rows, :], sin_ref[rows, :]
    lses, deltas = [], []
    for i in range(GROUP):
        at = slice(i * HEAD, (i + 1) * HEAD)
        kr[rows, at] = _turn(k_ref[rows, at].astype(jnp.float32), cos, sin).astype(jnp.bfloat16)
        qr[:, at] = _turn(q_ref[:, at].astype(jnp.float32), cos, sin).astype(jnp.bfloat16)
        lses.append(lse_ref[0, i : i + 1, :] * LOG2E)
        deltas.append((do_ref[:, at].astype(jnp.float32) * o_ref[:, at].astype(jnp.float32)).T.sum(axis=0, keepdims=True))
    dq_s[...] = jnp.zeros(dq_s.shape, jnp.float32)
    dk_s[rows, :] = jnp.zeros((BLOCK, wide), jnp.float32)
    dv_s[rows, :] = jnp.zeros((BLOCK, wide), jnp.float32)

    def block(first_key, keys, first_query, masked):
        here = pl.ds(first_key, keys)
        cols = slice(first_query, BLOCK)
        heads = [slice(i * HEAD, (i + 1) * HEAD) for i in range(GROUP)]
        scores = [_dot(kr[here, at], qr[cols, at], 1, 1) for at in heads]
        dps = [_dot(v_ref[here, at], do_ref[cols, at], 1, 1) for at in heads]
        ok = _hide(scores[0], 0, 0) if masked else None
        for i, at in enumerate(heads):
            p = jnp.exp2(scores[i] * e - lses[i][:, cols])
            if masked:
                p = jnp.where(ok, p, 0.0)
            ds = (p * (dps[i] - deltas[i][:, cols])).astype(jnp.bfloat16)
            dv_s[here, at] += _dot(p.astype(jnp.bfloat16), do_ref[cols, at], 1, 0)
            dk_s[here, at] += _dot(ds, qr[cols, at], 1, 0)
            dq_s[i, :, cols] += _dot(kr[here, at].T, ds, 1, 0)

    lax.fori_loop(0, iq, lambda j, _: block(pl.multiple_of(j * BLOCK, BLOCK), BLOCK, 0, False), None)
    for n in range(0, BLOCK, 256):
        block(pl.multiple_of(iq * BLOCK + n, 256), 256, n, True)

    def narrow(t):
        return t.astype(jnp.bfloat16).astype(jnp.float32)

    for i in range(GROUP):
        at = slice(i * HEAD, (i + 1) * HEAD)
        d_ref[rows, at] = _turn_back(narrow((dq_s[i] * scale).T), cos, sin).astype(jnp.bfloat16)

    @pl.when(iq == last)
    def _():
        def finish(n, _):
            here = pl.ds(pl.multiple_of(n * BLOCK, BLOCK), BLOCK)
            c, s = cos_ref[here, :], sin_ref[here, :]
            for i in range(GROUP):
                at = slice(i * HEAD, (i + 1) * HEAD)
                d_ref[here, wide + i * HEAD : wide + (i + 1) * HEAD] = _turn_back(narrow(dk_s[here, at] * scale), c, s).astype(jnp.bfloat16)
            d_ref[here, 2 * wide :] = dv_s[here, :].astype(jnp.bfloat16)

        lax.fori_loop(0, last + 1, finish, None)


def attend_bwd(qkv, o, do, lse, cos, sin):
    tokens, wide = qkv.shape[0], GROUP * HEAD
    groups = qkv.shape[1] // (3 * wide)
    table = pl.BlockSpec((tokens, HEAD), lambda g, i: (0, 0))
    own = pl.BlockSpec((BLOCK, wide), lambda g, i: (i, g))
    return pl.pallas_call(
        lambda *refs: _attend_bwd(*refs, scale=HEAD**-0.5),
        grid=(groups, tokens // BLOCK),
        in_specs=[
            pl.BlockSpec((BLOCK, wide), lambda g, i: (i, 3 * g)),
            pl.BlockSpec((tokens, wide), lambda g, i: (0, 3 * g + 1)),
            pl.BlockSpec((tokens, wide), lambda g, i: (0, 3 * g + 2)),
            own,
            own,
            pl.BlockSpec((1, GROUP, BLOCK), lambda g, i: (g, 0, i)),
            table,
            table,
        ],
        out_specs=pl.BlockSpec((tokens, 3 * wide), lambda g, i: (0, g)),
        out_shape=jax.ShapeDtypeStruct((tokens, groups * 3 * wide), jnp.bfloat16),
        scratch_shapes=[
            pltpu.VMEM((BLOCK, wide), jnp.bfloat16),
            pltpu.VMEM((tokens, wide), jnp.bfloat16),
            pltpu.VMEM((GROUP, HEAD, BLOCK), jnp.float32),
            pltpu.VMEM((tokens, wide), jnp.float32),
            pltpu.VMEM((tokens, wide), jnp.float32),
        ],
        compiler_params=pltpu.CompilerParams(dimension_semantics=("arbitrary", "arbitrary"), vmem_limit_bytes=VMEM),
        cost_estimate=pl.CostEstimate(flops=groups * 30 * 10**9, transcendentals=groups * 10**7, bytes_accessed=groups * 20 * 2**20),
        name="attend_bwd",
    )(qkv, qkv, qkv, o, do, lse, cos, sin)


def _up(b_ref, wg_ref, wu_ref, gate_ref, up_ref, act_ref):
    rows = gate_ref.shape[0]
    b = b_ref[pl.ds(pl.multiple_of(pl.program_id(1) * rows, rows), rows), :]
    gate, up = _dot(b, wg_ref[...], 1, 0), _dot(b, wu_ref[...], 1, 0)
    gate_ref[...] = gate
    up_ref[...] = up
    act_ref[...] = (gate * jax.nn.sigmoid(gate) * up).astype(jnp.bfloat16)


UP = (2048, 256)
TILE = 256
CUT = 512


def _up_parts(b, w_gate):
    (tokens, d), ff = b.shape, w_gate.shape[1]
    rows, tile = UP
    weight = pl.BlockSpec((d, tile), lambda j, i: (0, j))
    out = pl.BlockSpec((rows, tile), lambda j, i: (i, j))
    shapes = [jax.ShapeDtypeStruct((tokens, ff), t) for t in (jnp.float32, jnp.float32, jnp.bfloat16)]
    return (ff // tile, tokens // rows), [pl.BlockSpec((tokens, d), lambda j, i: (0, 0)), weight, weight], [out] * 3, shapes


def _up_cost(b, w_gate):
    (tokens, d), ff = b.shape, w_gate.shape[1]
    return pl.CostEstimate(flops=4 * tokens * d * ff, transcendentals=tokens * ff, bytes_accessed=10 * tokens * ff + 4 * d * ff)


def ffn_up(b, w_gate, w_up):
    grid, ins, outs, shapes = _up_parts(b, w_gate)
    return pl.pallas_call(
        _up,
        grid=grid,
        in_specs=ins,
        out_specs=outs,
        out_shape=shapes,
        compiler_params=pltpu.CompilerParams(dimension_semantics=("arbitrary",) * 2, vmem_limit_bytes=VMEM),
        cost_estimate=_up_cost(b, w_gate),
        name="ffn_up",
    )(b, w_gate, w_up)


def _ffn_bwd(dh_ref, wd_ref, gate_ref, up_ref, b_ref, dg_ref, du_ref, wg_ref, wu_ref, turned):
    @pl.when(pl.program_id(0) == 0)
    def _():
        for at in range(0, b_ref.shape[0], CUT):
            turned[:, at : at + CUT] = b_ref[at : at + CUT, :].T

    for at in range(0, dh_ref.shape[0], CUT):
        here = slice(at, at + CUT)
        dact = _dot(dh_ref[here, :], wd_ref[...], 1, 1).astype(jnp.bfloat16).astype(jnp.float32)
        gate, up = gate_ref[here, :], up_ref[here, :]
        s = jax.nn.sigmoid(gate)
        silu = gate * s
        du_ref[here, :] = (dact * silu).astype(jnp.bfloat16)
        dg_ref[here, :] = (dact * up * (s + silu * (1 - s))).astype(jnp.bfloat16)
    wg_ref[...] = _dot(turned[...], dg_ref[...], 1, 0).astype(jnp.bfloat16)
    wu_ref[...] = _dot(turned[...], du_ref[...], 1, 0).astype(jnp.bfloat16)


def _ffn_bwd_and_sum(dh_ref, wd_ref, gate_ref, up_ref, b_ref, term, dg_ref, du_ref, wg_ref, wu_ref, out, turned, *scratch):
    run = _reduction(term, out, *scratch)
    run(pl.program_id(0), pl.num_programs(0), lambda: _ffn_bwd(dh_ref, wd_ref, gate_ref, up_ref, b_ref, dg_ref, du_ref, wg_ref, wu_ref, turned))


def ffn_bwd(dh, w_down, gate, up, b, term=None, devices=None, number=None):
    (tokens, d), ff = dh.shape, w_down.shape[0]
    held = pl.BlockSpec((tokens, d), lambda j: (0, 0))
    cut, grad = pl.BlockSpec((tokens, TILE), lambda j: (0, j)), pl.BlockSpec((d, TILE), lambda j: (0, j))
    ins, outs = [held, pl.BlockSpec((TILE, d), lambda j: (j, 0)), cut, cut, held], [cut, cut, grad, grad]
    shapes = [jax.ShapeDtypeStruct((tokens, ff), jnp.bfloat16)] * 2 + [jax.ShapeDtypeStruct((d, ff), jnp.bfloat16)] * 2
    scratch, more, given = [pltpu.VMEM((d, tokens), jnp.bfloat16)], {}, [dh, w_down, gate, up, b]
    if term is not None:
        block = (term.shape[0] // devices, term.shape[1])
        ins, outs = ins + [pl.BlockSpec(memory_space=pl.ANY)], outs + [pl.BlockSpec(memory_space=pl.ANY)]
        shapes, scratch = shapes + [jax.ShapeDtypeStruct(block, jnp.bfloat16)], scratch + _reduction_scratch(*block)
        more, given = {"collective_id": number, "has_side_effects": True}, given + [term]
    return pl.pallas_call(
        _ffn_bwd if term is None else _ffn_bwd_and_sum,
        grid=(ff // TILE,),
        in_specs=ins,
        out_specs=outs,
        out_shape=shapes,
        scratch_shapes=scratch,
        compiler_params=pltpu.CompilerParams(dimension_semantics=("arbitrary",), vmem_limit_bytes=VMEM, **more),
        cost_estimate=pl.CostEstimate(flops=6 * tokens * d * ff, transcendentals=tokens * ff, bytes_accessed=12 * tokens * ff + 6 * d * ff),
        name="ffn_bwd",
    )(*given)


def matmul(a, w):
    return jnp.dot(a, w, preferred_element_type=jnp.float32).astype(jnp.bfloat16)


def matmul_nt(a, w):
    return _dot(a, w, 1, 1).astype(jnp.bfloat16)


def matmul_tn(a, b):
    return _dot(a, b, 0, 0).astype(jnp.bfloat16)


def norm_scale(h):
    return lax.rsqrt(jnp.mean(h.astype(jnp.float32) ** 2, -1, keepdims=True) + EPS)


def normed(h):
    return (h.astype(jnp.float32) * norm_scale(h)).astype(jnp.bfloat16)


def normed_bwd(h, da, dh):
    wide, da = h.astype(jnp.float32), da.astype(jnp.float32)
    scale = norm_scale(h)
    inner = jnp.sum(da * wide, -1, keepdims=True) * (scale**3 / h.shape[-1])
    return (dh.astype(jnp.float32) + (da * scale - wide * inner).astype(jnp.bfloat16).astype(jnp.float32)).astype(jnp.bfloat16)


def tables(tokens):
    half = HEAD // 2
    angle = jnp.arange(tokens, dtype=jnp.float32)[:, None] * THETA ** (-jnp.arange(half, dtype=jnp.float32) / half)
    cos, sin = jnp.cos(angle), jnp.sin(angle)
    return jnp.concatenate([cos, cos], -1), jnp.concatenate([-sin, sin], -1)


CHUNKS = 4


def _exchange(refs, out, stage, sems, *, layer, pieces):
    loaded, own, sends, recvs = sems
    rep, dp = lax.axis_index("rep"), lax.axis_index("dp")
    x, core = dp // 2, dp % 2
    across = (rep, dp + 2 - 4 * x)
    group = (1 - rep, dp)
    partner = (rep, dp + 1 - 2 * core)
    rows = refs[0].shape[1]
    half = rows // 2
    part = half // CHUNKS

    def local():
        return [
            pltpu.make_async_copy(refs[i].at[layer, :, pl.ds(at, wide)], stage.at[:, pl.ds(to, wide)], loaded.at[n])
            for n, (i, at, wide, to) in enumerate(pieces)
        ]

    def remote(source, at, size, n, device):
        return pltpu.make_async_remote_copy(
            src_ref=source, dst_ref=out.at[pl.ds(at, size), :], send_sem=sends.at[n], recv_sem=recvs.at[n],
            device_id=device, device_id_type=pl.DeviceIdType.MESH,
        )

    def block(of, rep_half, k):
        return of * rows + rep_half * half + k * part

    def first(k):
        return remote(stage.at[pl.ds(rep * half + k * part, part), :], block(dp, rep, k), part, k, across)

    def whole():
        return remote(stage, dp * rows, rows, 4 * CHUNKS, partner)

    def place():
        return pltpu.make_async_copy(stage, out.at[pl.ds(dp * rows, rows), :], own.at[0])

    theirs = dp + 2 - 4 * x

    def onward(k, rep_half, n, device):
        at = block(theirs, rep_half, k)
        return remote(out.at[pl.ds(at, part), :], at, part, n * CHUNKS + k, device)

    def start():
        for copy in local():
            copy.start()
        barrier = pltpu.get_barrier_semaphore()
        for device in (across, group, partner):
            pl.semaphore_signal(barrier, inc=1, device_id=device, device_id_type=pl.DeviceIdType.MESH)
        pl.semaphore_wait(barrier, 3)
        for copy in local():
            copy.wait()
        for k in range(CHUNKS):
            first(k).start()
        whole().start()
        place().start()

    def relay(k):
        first(k).wait_recv()
        onward(k, rep, 1, group).start()
        onward(k, rep, 2, partner).start()

    def relay_other(k):
        onward(k, rep, 1, group).wait_recv()
        onward(k, 1 - rep, 3, partner).start()

    def finish():
        place().wait()
        whole().wait()
        for k in range(CHUNKS):
            first(k).wait_send()
            onward(k, rep, 1, group).wait_send()
            onward(k, rep, 2, partner).wait()
            onward(k, 1 - rep, 3, partner).wait()

    return start, relay, relay_other, finish


def _exchange_scratch(rows, columns, pieces):
    return [
        pltpu.VMEM((rows, columns), jnp.bfloat16),
        pltpu.SemaphoreType.DMA((len(pieces),)),
        pltpu.SemaphoreType.DMA((1,)),
        pltpu.SemaphoreType.DMA((4 * CHUNKS + 1,)),
        pltpu.SemaphoreType.DMA((4 * CHUNKS + 1,)),
    ]


def _interleaved(columns):
    wide = GROUP * HEAD
    return [(i, a, wide, 3 * a + i * wide) for a in range(0, columns, wide) for i in range(3)]


def _fetch(wq, wk, wv, out, stage, *sems, layer):
    pieces = _interleaved(wq.shape[2])
    start, relay, relay_other, finish = _exchange((wq, wk, wv), out, stage, sems, layer=layer, pieces=pieces)
    start()
    relay(0)
    for k in range(1, CHUNKS):
        relay(k)
        relay_other(k - 1)
    relay_other(CHUNKS - 1)
    finish()


def fetch(wq, wk, wv, layer, devices):
    rows, columns = wq.shape[1], 3 * wq.shape[2]
    return pl.pallas_call(
        lambda *refs: _fetch(*refs, layer=layer),
        in_specs=[pl.BlockSpec(memory_space=pl.ANY)] * 3,
        out_specs=pl.BlockSpec(memory_space=pl.ANY),
        out_shape=jax.ShapeDtypeStruct((devices * rows, columns), jnp.bfloat16),
        scratch_shapes=_exchange_scratch(rows, columns, _interleaved(wq.shape[2])),
        compiler_params=pltpu.CompilerParams(collective_id=layer, has_side_effects=True),
        cost_estimate=pl.CostEstimate(flops=20 * 10**9, transcendentals=0, bytes_accessed=2 * devices * rows * columns),
        name="fetch",
    )(wq, wk, wv)


def _attend_and_fetch(q_ref, k_ref, v_ref, cos_ref, sin_ref, wo, o_ref, lse_ref, out, qr, kr, top_s, mix_s, stage, *sems, layer):
    steps = pl.num_programs(0) * pl.num_programs(1)
    step = pl.program_id(0) * pl.num_programs(1) + pl.program_id(1)
    pieces = [(0, 0, wo.shape[2], 0)]
    start, relay, relay_other, finish = _exchange((wo,), out, stage, sems, layer=layer, pieces=pieces)
    pl.when(step == 0)(start)
    for k in range(CHUNKS):
        pl.when(step == steps // 2)(lambda k=k: relay(k))
        pl.when(step == steps - 2)(lambda k=k: relay_other(k))
    _attend(q_ref, k_ref, v_ref, cos_ref, sin_ref, o_ref, lse_ref, qr, kr, top_s, mix_s, scale=HEAD**-0.5)
    pl.when(step == steps - 1)(finish)


def attend_and_fetch(qkv, cos, sin, wo, layer, devices, number):
    tokens, wide = qkv.shape[0], GROUP * HEAD
    groups = qkv.shape[1] // (3 * wide)
    table = pl.BlockSpec((tokens, HEAD), lambda g, i: (0, 0))
    anywhere = pl.BlockSpec(memory_space=pl.ANY)
    rows, columns = wo.shape[1:]
    return pl.pallas_call(
        lambda *refs: _attend_and_fetch(*refs, layer=layer),
        grid=(groups, tokens // BLOCK),
        in_specs=[
            pl.BlockSpec((BLOCK, wide), lambda g, i: (i, 3 * g)),
            pl.BlockSpec((tokens, wide), lambda g, i: (0, 3 * g + 1)),
            pl.BlockSpec((tokens, wide), lambda g, i: (0, 3 * g + 2)),
            table,
            table,
            anywhere,
        ],
        out_specs=[pl.BlockSpec((BLOCK, wide), lambda g, i: (i, g)), pl.BlockSpec((1, GROUP, BLOCK), lambda g, i: (g, 0, i)), anywhere],
        out_shape=[
            jax.ShapeDtypeStruct((tokens, groups * wide), jnp.bfloat16),
            jax.ShapeDtypeStruct((groups, GROUP, tokens), jnp.float32),
            jax.ShapeDtypeStruct((devices * rows, columns), jnp.bfloat16),
        ],
        scratch_shapes=[
            pltpu.VMEM((BLOCK, wide), jnp.bfloat16),
            pltpu.VMEM((tokens, wide), jnp.bfloat16),
            pltpu.VMEM((8, BLOCK), jnp.float32),
            pltpu.VMEM((GROUP, HEAD + 8, BLOCK), jnp.float32),
        ]
        + _exchange_scratch(rows, columns, [0]),
        compiler_params=pltpu.CompilerParams(
            dimension_semantics=("arbitrary", "arbitrary"), vmem_limit_bytes=VMEM, collective_id=number, has_side_effects=True
        ),
        cost_estimate=pl.CostEstimate(flops=30 * 10**9, transcendentals=20 * 10**6, bytes_accessed=20 * 2**20),
        name="attend",
    )(qkv, qkv, qkv, cos, sin, wo)


def _up_and_fetch(b_ref, wg_ref, wu_ref, wq, wk, wv, gate_ref, up_ref, act_ref, out, stage, *sems, layer):
    step, last = pl.program_id(0) * pl.num_programs(1) + pl.program_id(1), pl.num_programs(0) * pl.num_programs(1) - 1
    start, relay, relay_other, finish = _exchange((wq, wk, wv), out, stage, sems, layer=layer, pieces=_interleaved(wq.shape[2]))
    pl.when(step == 0)(start)
    for k in range(CHUNKS):
        pl.when(step == 3 + 3 * k)(lambda k=k: relay(k))
        pl.when(step == 5 + 3 * k)(lambda k=k: relay_other(k))
    _up(b_ref, wg_ref, wu_ref, gate_ref, up_ref, act_ref)
    pl.when(step == last)(finish)


def ffn_up_and_fetch(b, w_gate, w_up, wq, wk, wv, layer):
    grid, ins, outs, shapes = _up_parts(b, w_gate)
    own, columns = wq.shape[1], 3 * wq.shape[2]
    anywhere = pl.BlockSpec(memory_space=pl.ANY)
    return pl.pallas_call(
        lambda *refs: _up_and_fetch(*refs, layer=layer),
        grid=grid,
        in_specs=ins + [anywhere] * 3,
        out_specs=outs + [anywhere],
        out_shape=shapes + [jax.ShapeDtypeStruct((b.shape[1], columns), jnp.bfloat16)],
        scratch_shapes=_exchange_scratch(own, columns, _interleaved(wq.shape[2])),
        compiler_params=pltpu.CompilerParams(
            dimension_semantics=("arbitrary",) * 2, vmem_limit_bytes=VMEM, collective_id=layer, has_side_effects=True
        ),
        cost_estimate=_up_cost(b, w_gate),
        name="ffn_up_and_fetch",
    )(b, w_gate, w_up, wq, wk, wv)


PARTS = 4


def _reduction(term, out, mine, partners, total, theirs, loaded, sends, recvs):
    rows = out.shape[0]
    part = rows // PARTS
    rep, dp = lax.axis_index("rep"), lax.axis_index("dp")
    x, core = dp // 2, dp % 2
    across, partner = (rep, dp + 2 - 4 * x), (rep, dp + 1 - 2 * core)

    def remote(source, target, n, device):
        return pltpu.make_async_remote_copy(
            src_ref=source, dst_ref=target, send_sem=sends.at[n], recv_sem=recvs.at[n],
            device_id=device, device_id_type=pl.DeviceIdType.MESH,
        )

    def of(block, k):
        owner = (1 - x if block == 0 else x) * 2
        return owner * rows + k * part

    def here(k):
        return pl.ds(k * part, part)

    def load(block, k):
        return pltpu.make_async_copy(term.at[pl.ds(of(block, k) + core * rows, part), :], mine.at[block, here(k), :], loaded.at[block * PARTS + k])

    def give(block, k):
        source = term.at[pl.ds(of(block, k) + (1 - core) * rows, part), :]
        return remote(source, partners.at[block, here(k), :], block * PARTS + k, partner)

    def send(k):
        return remote(total.at[here(k), :], theirs.at[here(k), :], 2 * PARTS + k, across)

    def put(k):
        return pltpu.make_async_copy(mine.at[1, here(k), :], out.at[here(k), :], loaded.at[2 * PARTS + k])

    def start():
        barrier = pltpu.get_barrier_semaphore()
        for device in (across, partner):
            pl.semaphore_signal(barrier, inc=1, device_id=device, device_id_type=pl.DeviceIdType.MESH)
        for block in range(2):
            for k in range(PARTS):
                load(block, k).start()
        pl.semaphore_wait(barrier, 2)
        for block in range(2):
            for k in range(PARTS):
                give(block, k).start()

    def add(k):
        load(0, k).wait()
        give(0, k).wait_recv()
        total[here(k), :] = (mine[0, here(k), :].astype(jnp.float32) + partners[0, here(k), :].astype(jnp.float32)).astype(jnp.bfloat16)

    def close(k):
        load(1, k).wait()
        give(1, k).wait_recv()
        send(k).wait_recv()
        own = mine[1, here(k), :].astype(jnp.float32) + partners[1, here(k), :].astype(jnp.float32)
        mine[1, here(k), :] = (own + theirs[here(k), :].astype(jnp.float32)).astype(jnp.bfloat16)

    def finish():
        for k in range(PARTS):
            put(k).wait()
            send(k).wait_send()
            for block in range(2):
                give(block, k).wait_send()

    def run(step, steps, body):
        pl.when(step == 0)(start)
        for k in range(PARTS):
            pl.when(step == 1 + k)(lambda k=k: add(k))
            pl.when(step == 2 + k)(lambda k=k: send(k).start())
        for k in range(PARTS - 1):
            at = steps - 8 + 3 * k
            pl.when(step == at)(lambda k=k: close(k))
            pl.when(step == at + 1)(lambda k=k: put(k).start())
        body()

        @pl.when(step == steps - 1)
        def _():
            close(PARTS - 1)
            put(PARTS - 1).start()
            finish()

    return run


def _reduction_scratch(rows, columns):
    return [
        pltpu.VMEM((2, rows, columns), jnp.bfloat16),
        pltpu.VMEM((2, rows, columns), jnp.bfloat16),
        pltpu.VMEM((rows, columns), jnp.bfloat16),
        pltpu.VMEM((rows, columns), jnp.bfloat16),
        pltpu.SemaphoreType.DMA((3 * PARTS,)),
        pltpu.SemaphoreType.DMA((3 * PARTS,)),
        pltpu.SemaphoreType.DMA((3 * PARTS,)),
    ]


def parted(t):
    wide = GROUP * HEAD
    return [jnp.concatenate([t[:, a : a + wide] for a in range(n * wide, t.shape[1], 3 * wide)], axis=1) for n in range(3)]


def together(first, *rest):
    return lax.optimization_barrier((first, *rest))


def solution(mesh):
    reps = mesh.shape["rep"]

    def step(x, dy, *weights):
        layers = weights[0].shape[0]
        rep = lax.axis_index("rep")
        cos, sin = tables(x.shape[1])

        def mine(w, number):
            part = w.shape[1] // reps
            return lax.dynamic_slice(w, (number, rep * part, 0), (1, part, w.shape[2]))[0]

        def whole(shard):
            return lax.all_gather(shard, ("dp", "rep"), axis=0, tiled=True)

        def scatter(term):
            return lax.psum_scatter(term, "dp", scatter_dimension=0, tiled=True)

        fetched = []
        for n in range(layers):
            fetched.append([whole(mine(w, n)) for w in weights[4:]])

        h, kept = x[0], []
        square = fetch(*weights[:3], 0, mesh.shape["dp"])
        for n in range(layers):
            wg, wu, wd = fetched[n]
            a = normed(h)
            qkv = matmul(a, square)
            o, lse, wo = attend_and_fetch(qkv, cos, sin, weights[3], n, mesh.shape["dp"], 2 * layers + n)
            h1 = h + matmul(o, wo)
            b = normed(h1)
            held = square
            if n < layers - 1:
                gate, up, act, square = ffn_up_and_fetch(b, wg, wu, *weights[:3], n + 1)
            else:
                gate, up, act = ffn_up(b, wg, wu)
            kept.append((h, a, qkv, o, lse, h1, b, gate, up, act, held, wo))
            if n < layers - 1:
                h = h1 + matmul(act, wd)

        dh, grads, sums, out = dy[0], [None] * layers, {}, {}

        def after(value, *keys):
            for key in keys:
                if key in sums:
                    value, out[key] = together(value, sums.pop(key))
            return value

        for n in reversed(range(layers)):
            wg, wu, wd = fetched[n]
            h, a, qkv, o, lse, h1, b, gate, up, act, square, wo = kept[n]
            dh = after(dh, ("up", n + 1))
            d_down = matmul_tn(act, dh)
            dh, d_down = together(dh, d_down)
            dg, du, d_gate, d_up, out["down", n] = ffn_bwd(dh, wd, gate, up, b, d_down, mesh.shape["dp"], layers + n)
            dg = after(dg, ("o", n + 1), ("qkv", n + 1))
            sums["gate", n], sums["up", n] = scatter(d_gate), scatter(d_up)
            db = matmul_nt(dg, wg) + matmul_nt(du, wu)
            dh1 = normed_bwd(h1, db, dh)
            d_o = matmul_tn(o, dh1)
            dh1, d_o = together(dh1, d_o)
            sums["o", n] = scatter(d_o)
            do = matmul_nt(dh1, wo)
            dqkv = after(attend_bwd(qkv, o, do, lse, cos, sin), ("gate", n))
            d_qkv = matmul_tn(a, dqkv)
            dqkv, d_qkv = together(dqkv, d_qkv)
            sums["qkv", n] = scatter(d_qkv)
            da = matmul_nt(dqkv, square)
            dh = normed_bwd(h, da, dh1)
        out |= sums
        grads = []
        for n in range(layers):
            grads.append((*parted(out["qkv", n]), *(out[name, n] for name in ("o", "gate", "up", "down"))))
        return (dh[None], *(jnp.stack([g[i] for g in grads]) for i in range(7)))

    states, cut = P(("rep", "dp"), None, None), P(None, "dp", None)
    return jax.shard_map(
        step,
        mesh=mesh,
        in_specs=(states, states) + (cut,) * 7,
        out_specs=(states,) + (P("rep", "dp", None),) * 7,
        check_vma=False,
    )
```
